32 devices in a mesh: cuts: 8 (over z, y), event: 4 (over x, core).
Axes of the slice: x: 2, y: 2, z: 4, core: 2. Of those that a mesh axis runs over, the one named last changes fastest.
Arguments:
- kernels: float32 [4, 64, 128, 256], P('event', 'cuts'), may hold values from -24 to 24
- steps: float32 [8, 64, 128, 256], P(None, 'cuts', 'event'), may hold values from -11 to 11
- curvature: float32 [8, 64, 128, 256], P(None, 'cuts', 'event'), may hold values from 0.2 to 5
Outputs:
- gradient: float32 [64, 128, 256], P('cuts', 'event')
- direction: float32 [64, 128, 256], P('cuts', 'event')
The draws below stay inside these ranges and needn't reach their ends.
All inputs are finite; a program needn't handle non-finite values.
Results may differ from the reference program's by a relative error of at most 0.00021.
Values sent between devices are 32-bit elements; how exact they have to be, the bound alone decides.
A program may use at most 64 MiB of HBM per device.

```python
import math
import jax
import jax.numpy as jnp
from jax import lax

NR = 128
NB = 256
PAIRS = 8
RIM = 4
NA = 64
GROUPS = 4


def band_matrix(length, sigma):
    points = jnp.arange(length, dtype=jnp.float32)
    offset = points[:, None] - points[None, :]
    return jnp.exp(-offset * offset / (2.0 * sigma * sigma))


def circle_matrix(length, sigma):
    points = jnp.arange(length, dtype=jnp.float32)
    offset = jnp.abs(points[:, None] - points[None, :])
    offset = jnp.minimum(offset, length - offset)
    return jnp.exp(-offset * offset / (2.0 * sigma * sigma))


def shared_field(key):
    white = jax.random.truncated_normal(jax.random.fold_in(key, 101), -4.0, 4.0, (NA, NR, NB), jnp.float32)
    lon_mat = circle_matrix(NA, 3.0)
    rad_mat = band_matrix(NR, max(2.0, NR / 16.0))
    lat_mat = band_matrix(NB, max(2.0, NB / 32.0))
    field = jnp.einsum('ia,ajb->ijb', lon_mat, white, precision=lax.Precision.HIGHEST)
    field = jnp.einsum('rj,ajb->arb', rad_mat, field, precision=lax.Precision.HIGHEST)
    field = jnp.einsum('ajb,cb->ajc', field, lat_mat, precision=lax.Precision.HIGHEST)
    field = field / jnp.sqrt(jnp.mean(field * field))
    field = jnp.clip(field, -4.0, 4.0)
    return field


def draw_kernels(key, part):
    field = shared_field(key)
    gains = jax.random.uniform(jax.random.fold_in(key, 202), (GROUPS,), jnp.float32, 0.5, 1.5)
    noise = 4.0 * jax.random.truncated_normal(jax.random.fold_in(key, 203), -4.0, 4.0, (GROUPS, NA, NR, NB), jnp.float32)
    return gains[:, None, None, None] * field[None] + noise


def draw_steps(key, part):
    field = shared_field(key)
    factors = jax.random.uniform(jax.random.fold_in(key, 303), (PAIRS,), jnp.float32, 0.3, 1.5)
    noise = jax.random.truncated_normal(jax.random.fold_in(key, 304), -4.0, 4.0, (PAIRS, NA, NR, NB), jnp.float32)
    return -factors[:, None, None, None] * field[None] + noise


def levels(rng, dims, split, smallest, top_value):
    factor_of, own = 1.0, jax.random.fold_in(rng, 6)
    for dim, parts in split:
        steps = jnp.exp(jax.random.uniform(jax.random.fold_in(own, dim), (parts,), jnp.float32, smallest / len(split), top_value / len(split)))
        factor_of = factor_of * jnp.repeat(steps, dims[dim] // parts).reshape([-1 if axis == dim else 1 for axis in range(len(dims))])
    return factor_of


def setup_inputs(seed: int = 0) -> dict:
    streams_of = jax.random.split(jax.random.key(seed), 4)
    kernels = draw_kernels(jax.random.fold_in(streams_of[3], 71), 0)
    steps = draw_steps(jax.random.fold_in(streams_of[3], 71), 0)
    curvature = jnp.clip(jnp.exp(math.log(5.0) - 3.218876 * jax.random.uniform(streams_of[2], (PAIRS, NA, NR, NB), jnp.float32) ** levels(streams_of[2], (PAIRS, NA, NR, NB), ((1, 8), (2, 4)), -0.2, 0.2)), 0.2, 5.0)
    return {"kernels": kernels, "steps": steps, "curvature": curvature}


def gauss_matrix(length, sigma):
    points = jnp.arange(length, dtype=jnp.float32)
    offset = points[:, None] - points[None, :]
    matrix = jnp.exp(-offset * offset / (2.0 * sigma * sigma))
    return matrix / jnp.sum(matrix, axis=1, keepdims=True)


def cycle_weights():
    unscaled = [math.exp(-((column - RIM) ** 2) / 4.5) for column in range(2 * RIM + 1)]
    whole = sum(unscaled)
    return [weight / whole for weight in unscaled]


def reference(kernels, steps, curvature):
    summed = jnp.sum(kernels, axis=0)
    radial = jnp.einsum("ij,ajb->aib", gauss_matrix(summed.shape[1], 3.0), summed, precision=lax.Precision.HIGHEST)
    lat_len = radial.shape[2]
    plane = jnp.dot(radial.reshape(-1, lat_len), gauss_matrix(lat_len, 4.0).T, precision=lax.Precision.HIGHEST).reshape(radial.shape)
    weights = cycle_weights()
    gradient = jnp.zeros_like(plane)
    for column in range(2 * RIM + 1):
        gradient = gradient + weights[column] * jnp.roll(plane, RIM - column, axis=0)
    changes = curvature * steps
    curvs = jnp.sum(changes * steps, axis=(1, 2, 3))
    inverse = 1.0 / curvs
    scaling = curvs[PAIRS - 1] / jnp.sum(changes[PAIRS - 1] * changes[PAIRS - 1])
    carried = gradient
    alphas = [None] * PAIRS
    for pair in reversed(range(PAIRS)):
        alphas[pair] = inverse[pair] * jnp.sum(steps[pair] * carried)
        carried = carried - alphas[pair] * changes[pair]
    result = scaling * carried
    for pair in range(PAIRS):
        second = inverse[pair] * jnp.sum(changes[pair] * result)
        result = result + (alphas[pair] - second) * steps[pair]
    return gradient, -result
```

```python
import functools
import math

import jax
import jax.numpy as jnp
from jax import lax
from jax.experimental import pallas as pl
from jax.experimental.pallas import tpu as pltpu
from jax.sharding import PartitionSpec as P

RIM = 4
LOADS = 4
LANES = 128
SUB = 8
MESH = pl.DeviceIdType.MESH
HIGHEST = lax.Precision.HIGHEST


def cycle_weights():
    unscaled = [math.exp(-((column - RIM) ** 2) / 4.5) for column in range(2 * RIM + 1)]
    whole = sum(unscaled)
    return [weight / whole for weight in unscaled]


def halves(value):
    high = value.astype(jnp.bfloat16)
    return high, (value - high.astype(jnp.float32)).astype(jnp.bfloat16)


def unscaled_gauss(length, sigma):
    rows = lax.broadcasted_iota(jnp.int32, (length, length), 0)
    columns = lax.broadcasted_iota(jnp.int32, (length, length), 1)
    offset = (rows - columns).astype(jnp.float32)
    return jnp.exp(-offset * offset / (2.0 * sigma * sigma))


def factor(shape, spot_axis, length, sigma, count):
    reach = 2.25 * sigma
    pitch = (length - 1 + 2 * reach) / (count - 1)
    assert pitch < 0.54 * sigma
    spots = lax.broadcasted_iota(jnp.int32, shape, spot_axis).astype(jnp.float32)
    nodes = lax.broadcasted_iota(jnp.int32, shape, 1 - spot_axis).astype(jnp.float32)
    offset = spots - (nodes * pitch - reach)
    return jnp.exp(-offset * offset / (sigma * sigma))


def upper(pairs):
    return [(i, j) for i in range(pairs) for j in range(i, pairs)]


def kernel(
    sizes,
    kern_hbm, steps_hbm, curv_hbm, grad, steps, changes, coef,
    kern, rad, far_in, near_in, far_out, x_in, nodes, halo_in, smooth, short,
    rad_mat, pack_mat, dual_mat, lat_mat, gram_acc, gram_row, gram_all,
    table, splat, mix, late_row, late_all,
    ready, load_sem, core_send, core_recv, x_send, x_recv, halo_send, halo_recv,
    gram_send, gram_recv, late_send, late_recv,
):
    n_c, n_e, pairs, rad_len, lat_len = sizes
    part = rad_len // n_e
    c = lax.axis_index("cuts")
    e = lax.axis_index("event")
    barrier = pltpu.get_barrier_semaphore()
    steps_left, steps_right = c >= 2, c + 2 < n_c
    rounds = n_c // 2

    def flip(place):
        return c + place * (1 - 2 * lax.rem(c // place, 2))

    def greet(semaphore):
        for d in range(1, n_e):
            pl.semaphore_signal(
                semaphore, 1, device_id={"event": lax.rem(e + d, n_e)}, device_id_type=MESH
            )
        pl.semaphore_signal(semaphore, 1, device_id={"cuts": flip(1)}, device_id_type=MESH)

        @pl.when(steps_left)
        def _():
            pl.semaphore_signal(semaphore, 1, device_id={"cuts": c - 2}, device_id_type=MESH)

        @pl.when(steps_right)
        def _():
            pl.semaphore_signal(semaphore, 1, device_id={"cuts": c + 2}, device_id_type=MESH)

    def greeted(semaphore):
        pl.semaphore_wait(
            semaphore, n_e + steps_left.astype(jnp.int32) + steps_right.astype(jnp.int32)
        )

    def relay(number):
        greeted(ready.at[number - 1] if number else barrier)
        if number < rounds:
            greet(ready.at[number])

    greet(barrier)
    others = []
    for mask in reversed(range(n_c)):
        where = c
        for bit in range(mask.bit_length()):
            if mask >> bit & 1:
                where = where + (flip(1 << bit) - c)
        for d in range(n_e):
            if mask or d:
                others.append({"cuts": where, "event": lax.rem(e + d, n_e)})

    per = 2 * RIM // LOADS
    loads = []
    for p in range(LOADS):
        side, ks = p * per // RIM, pl.ds(p * per % RIM, per)
        loads.append(pltpu.make_async_copy(
            kern_hbm.at[side, ks], kern.at[side, ks], load_sem.at[p]
        ))
        loads[-1].start()
    loads.append(pltpu.make_async_copy(steps_hbm, steps, load_sem.at[LOADS]))
    loads.append(pltpu.make_async_copy(curv_hbm, changes, load_sem.at[LOADS + 1]))

    matrix = unscaled_gauss(rad_len, 3.0)
    high, low = halves(matrix / jnp.sum(matrix, axis=1, keepdims=True))
    rad_mat[...] = jnp.concatenate([high, high, low], axis=1)
    spread_out = factor((lat_len, LANES), 0, lat_len, 4.0, LANES)
    high, low = halves(spread_out)
    both = jnp.concatenate([high, low], axis=1)
    pack_mat[...] = jnp.concatenate([both, both], axis=0)
    table[...] = jnp.zeros_like(table)

    core = e + 1 - 2 * lax.rem(e, 2)
    far = lax.rem(e + 2, n_e)
    core_far = lax.rem(core + 2, n_e)

    def rows(chunk):
        return pl.ds(pl.multiple_of(chunk * part, part), part)

    def send(src, dst, send_sem, recv_sem, where):
        return pltpu.make_async_remote_copy(
            src_ref=src, dst_ref=dst, send_sem=send_sem, recv_sem=recv_sem,
            device_id=where, device_id_type=MESH,
        )

    far_copies, near_copies, x_copies, halo_copies = [], [], [], []

    def packed(value, matrix):
        high, low = halves(value)
        out = jnp.dot(
            jnp.concatenate([high, low], axis=1), matrix[...], preferred_element_type=jnp.float32
        )
        return out[:, :LANES] + out[:, LANES:]

    for p in range(LOADS):
        side, first = p * per // RIM, p * per % RIM
        loads[p].wait()
        if p == LOADS - 1:
            for load in loads[LOADS:]:
                load.start()
        value = packed(
            kern[side, pl.ds(first, per)].reshape(per * rad_len, lat_len), pack_mat
        ).reshape(per, rad_len, LANES)
        high, low = halves(jnp.concatenate([value[k] for k in range(per)], axis=1))
        value = jnp.dot(
            rad_mat[...], jnp.concatenate([high, low, high], axis=0),
            preferred_element_type=jnp.float32,
        )
        for k in range(per):
            rad[side, first + k] = value[:, k * LANES : (k + 1) * LANES]
    relay(0)
    for number, (copies, chunk, into) in enumerate(
        ((far_copies, core_far, far_in), (near_copies, core, near_in))
    ):
        for p in range(LOADS):
            side, ks = p * per // RIM, pl.ds(p * per % RIM, per)
            copies.append(send(
                rad.at[side, ks, rows(chunk)], into.at[side, ks],
                core_send.at[number, p], core_recv.at[number, p], {"event": core},
            ))
            copies[-1].start()
    strips = part // SUB
    pieces = [(h, g) for h in range(strips) for g in range(2)]

    def strip_rows(chunk, h):
        return pl.ds(pl.multiple_of(chunk * part + h * SUB, SUB), SUB)

    matrix = spread_out * jnp.sum(spread_out, axis=0, keepdims=True)
    high, low = halves(spread_out / jnp.sum(matrix, axis=1, keepdims=True))
    both = jnp.concatenate([high, low], axis=1)
    dual_mat[...] = jnp.concatenate([both, both], axis=0)
    matrix = factor((LANES, lat_len), 1, lat_len, 4.0, LANES)
    whole = jnp.sum(matrix * jnp.sum(matrix, axis=1, keepdims=True), axis=0, keepdims=True)
    high, low = halves(matrix / whole)
    lat_mat[...] = jnp.concatenate([high, high, low], axis=0)

    for copy in far_copies:
        copy.wait_recv()
    for h, g in pieces:
        here = pl.ds(h * SUB, SUB)
        far_out[g, :, here] = rad[g, :, strip_rows(far, h)] + far_in[g, :, here]
        x_copies.append(send(
            far_out.at[g, :, here], x_in.at[g, :, here], x_send.at[h, g], x_recv.at[h, g],
            {"event": far},
        ))
        x_copies[-1].start()
    relay(1)

    slots = {pair: number for number, pair in enumerate(upper(pairs))}
    count = len(slots)
    groups = [(0, 1), (2, 3), tuple(range(4, pairs))]
    all_rows = steps.shape[1]
    tiles = all_rows // SUB
    lats = lat_len // LANES
    strip = tiles // RIM

    def gram(number):
        if number == 0:
            loads[LOADS].wait()
            loads[LOADS + 1].wait()

        def scale(t, _):
            place = pl.ds(pl.multiple_of(t * SUB, SUB), SUB)
            for i in range(pairs):
                changes[i, place, :] = changes[i, place, :] * steps[i, place, :]
            return 0

        lax.fori_loop(number * strip, (number + 1) * strip, scale, 0, unroll=2)
        for group in groups:
            wanted = [(i, j) for i in group for j in range(i, pairs)]

            def body(t, sums):
                place = pl.ds(pl.multiple_of(t * SUB, SUB), SUB)
                sums = list(sums)
                for lane in range(lats):
                    across = pl.ds(lane * LANES, LANES)
                    change = {j: changes[j, place, across] for j in range(group[0], pairs)}
                    for n, i in enumerate(group):
                        step = steps[i, place, across]
                        for m, (a, b) in enumerate(wanted):
                            if a == i:
                                sums[2 * m] = sums[2 * m] + step * change[b]
                                sums[2 * m + 1] = sums[2 * m + 1] + change[i] * change[b]
                return tuple(sums)

            sums = lax.fori_loop(
                number * strip, (number + 1) * strip, body,
                tuple(jnp.zeros((SUB, LANES), jnp.float32) for _ in range(2 * len(wanted))),
            )
            for m, pair in enumerate(wanted):
                for kind in range(2):
                    place = slots[pair] + kind * count
                    if number == 0:
                        gram_acc[place] = sums[2 * m + kind]
                    else:
                        gram_acc[place] = gram_acc[place] + sums[2 * m + kind]

    def spread(row, slot_refs, sends, recvs):
        for d, other in enumerate(others):
            send(row, slot_refs.at[d], sends.at[d], recvs.at[d], other).start()
        return [
            send(row, slot_refs.at[d], sends.at[d], recvs.at[d], other)
            for d, other in enumerate(others)
        ]

    def gathered(row, slot_refs, copies):
        for copy in copies:
            copy.wait_recv()
        return row[...] + jnp.sum(slot_refs[...], axis=0)

    def arrive(h, g):
        here = pl.ds(h * SUB, SUB)
        base = rad[g, :, strip_rows(e, h)] + near_in[g, :, here]
        x_copies[2 * h + g].wait_recv()
        nodes[g, :, here] = base + x_in[g, :, here]
        halo_copies.append(send(
            nodes.at[g, :, here], halo_in.at[g, :, here], halo_send.at[h, g], halo_recv.at[h, g],
            {"cuts": lax.rem(c + n_c - 1 + 2 * g, n_c)},
        ))
        halo_copies[-1].start()

    def shorten(i):
        for kind, vector in enumerate((steps, changes)):
            short[kind * pairs + i] = packed(vector[i], dual_mat)

    weights = cycle_weights()
    lons = 2 * RIM

    def finish(h):
        for copy in halo_copies[2 * h : 2 * h + 2]:
            copy.wait_recv()
        place = pl.ds(h * SUB, SUB)
        padded = (
            [halo_in[1, k, place] for k in range(RIM)]
            + [nodes[side, k, place] for side in range(2) for k in range(RIM)]
            + [halo_in[0, k, place] for k in range(RIM)]
        )
        sums = [None] * (2 * pairs)
        for a in range(lons):
            value = weights[RIM] * padded[a + RIM]
            for k in range(1, RIM + 1):
                value = value + weights[RIM + k] * (padded[a + RIM - k] + padded[a + RIM + k])
            spot = pl.ds(a * part + h * SUB, SUB)
            smooth[spot, :] = value
            for n in range(2 * pairs):
                term = value * short[n, spot, :]
                sums[n] = term if sums[n] is None else sums[n] + term
        for n in range(2 * pairs):
            place = pl.ds(n * SUB, SUB)
            table[place, :] = sums[n] if h == 0 else table[place, :] + sums[n]

    gram(0)
    relay(2)
    gram(1)
    for number in range(3, rounds):
        relay(number)
    gram(2)
    gram(3)
    relay(rounds)
    ones = jnp.ones((LANES, LANES), jnp.float32)

    def lane_sums(value):
        return lax.dot_general(
            ones[:SUB], value, (((1,), (1,)), ((), ())), precision=HIGHEST,
            preferred_element_type=jnp.float32,
        )[:1]

    table[pl.ds(0, 2 * count), :] = jnp.sum(gram_acc[...], axis=1)
    gram_row[...] = lane_sums(table[...])
    gram_copies = spread(gram_row, gram_all, gram_send, gram_recv)
    for copy in near_copies:
        copy.wait_recv()
    for number, (h, g) in enumerate(pieces):
        arrive(h, g)
        for i in range(number * pairs // len(pieces), (number + 1) * pairs // len(pieces)):
            shorten(i)
    for h in range(strips):
        finish(h)
    first, _ = halves(table[...])
    second, third = halves(table[...] - first.astype(jnp.float32))
    late_row[...] = lax.dot_general(
        jnp.ones((SUB, 3 * LANES), jnp.bfloat16), jnp.concatenate([first, second, third], axis=1),
        (((1,), (1,)), ((), ())), preferred_element_type=jnp.float32,
    )[:1]
    late_copies = spread(late_row, late_all, late_send, late_recv)
    high, low = halves(smooth[...])
    grad[...] = jnp.dot(
        jnp.concatenate([high, low, high], axis=1), lat_mat[...],
        preferred_element_type=jnp.float32,
    )
    products = gathered(gram_row, gram_all, gram_copies)
    square = (LANES, LANES)
    on_diagonal = lax.broadcasted_iota(jnp.int32, square, 0) == lax.broadcasted_iota(jnp.int32, square, 1)
    splat[...] = jnp.dot(
        jnp.where(on_diagonal, jnp.broadcast_to(products, square), 0.0), ones,
        precision=HIGHEST, preferred_element_type=jnp.float32,
    )

    def cross(i, j):
        place = slots[i, j]
        return splat[place : place + 1, :]

    def squared(i, j):
        place = count + slots[min(i, j), max(i, j)]
        return splat[place : place + 1, :]

    def unit(place):
        return (lax.broadcasted_iota(jnp.int32, (1, LANES), 1) // SUB == place).astype(jnp.float32)

    inverse = [1.0 / cross(i, i) for i in range(pairs)]
    scaling = cross(pairs - 1, pairs - 1) / squared(pairs - 1, pairs - 1)
    alphas = [None] * pairs
    for i in reversed(range(pairs)):
        row = unit(i)
        for j in range(pairs - 1, i, -1):
            row = row - cross(i, j) * alphas[j]
        alphas[i] = inverse[i] * row
    onto = []
    for i in range(pairs):
        row = unit(pairs + i)
        for j in range(pairs):
            row = row - squared(i, j) * alphas[j]
        row = scaling * row
        for j in range(i):
            row = row + cross(j, i) * onto[j]
        onto.append(alphas[i] - inverse[i] * row)
    for i in range(pairs):
        mix[i : i + 1, :] = -onto[i]
        mix[pairs + i : pairs + i + 1, :] = scaling * alphas[i]

    for copies in (far_copies, near_copies, x_copies, halo_copies, gram_copies, late_copies):
        for copy in copies:
            copy.wait_send()
    products = gathered(late_row, late_all, late_copies)
    mixed = jnp.sum(mix[...] * products, axis=1, keepdims=True)
    coef[pl.ds(0, 2 * pairs), :] = jnp.broadcast_to(mixed, (2 * pairs, LANES))
    coef[pl.ds(2 * pairs, SUB), :] = jnp.broadcast_to(-scaling, (SUB, LANES))


def combine_kernel(pairs, blocks, grad, steps, changes, coef, grad_hbm, dir_hbm, direc, sems):
    grad_out = pltpu.make_async_copy(grad, grad_hbm, sems.at[blocks])
    grad_out.start()
    all_rows, lat_len = grad.shape
    ratio = jnp.broadcast_to(coef[2 * pairs : 2 * pairs + 1, :], (SUB, LANES))
    factors = [jnp.broadcast_to(coef[i : i + 1, :], (SUB, LANES)) for i in range(2 * pairs)]
    tiles = all_rows // SUB // blocks

    def combine(t, _):
        place = pl.ds(pl.multiple_of(t * SUB, SUB), SUB)
        for lane in range(lat_len // LANES):
            across = pl.ds(lane * LANES, LANES)
            value = ratio * grad[place, across]
            for i in range(pairs):
                value = value + factors[i] * steps[i, place, across]
                value = value + factors[pairs + i] * changes[i, place, across]
            direc[place, across] = value
        return 0

    copies = []
    for block in range(blocks):
        lax.fori_loop(block * tiles, (block + 1) * tiles, combine, 0, unroll=4)
        place = pl.ds(block * tiles * SUB, tiles * SUB)
        copies.append(pltpu.make_async_copy(direc.at[place], dir_hbm.at[place], sems.at[block]))
        copies[-1].start()
    grad_out.wait()
    for copy in copies:
        copy.wait()


def shards(kernels, steps, curvature):
    n_c, n_e = lax.axis_size("cuts"), lax.axis_size("event")
    _, lons, rad_len, lat_len = kernels.shape
    pairs = steps.shape[0]
    part = rad_len // n_e
    assert lons == 2 * RIM and n_e == 4 and n_c % 2 == 0
    all_rows = lons * part
    count = pairs * (pairs + 1)
    f32, bf16 = jnp.float32, jnp.bfloat16
    vmem, dma = pltpu.VMEM, pltpu.SemaphoreType.DMA
    whole = (2, RIM, part, LANES)
    vmem_spec = pl.BlockSpec(memory_space=pltpu.VMEM)
    any_spec = pl.BlockSpec(memory_space=pl.ANY)
    out = jax.ShapeDtypeStruct((all_rows, lat_len), f32)
    others = n_c * n_e - 1
    assert 2 * pairs * SUB == LANES
    staged = pl.pallas_call(
        functools.partial(kernel, (n_c, n_e, pairs, rad_len, lat_len)),
        out_shape=(
            vmem((all_rows, lat_len), f32),
            vmem((pairs, all_rows, lat_len), f32),
            vmem((pairs, all_rows, lat_len), f32),
            vmem((2 * pairs + SUB, LANES), f32),
        ),
        in_specs=[any_spec] * 3,
        out_specs=(vmem_spec,) * 4,
        scratch_shapes=[
            vmem((2, RIM, rad_len, lat_len), f32),
            vmem((2, RIM, rad_len, LANES), f32),
            vmem(whole, f32),
            vmem(whole, f32),
            vmem(whole, f32),
            vmem(whole, f32),
            vmem(whole, f32),
            vmem(whole, f32),
            vmem((all_rows, LANES), f32),
            vmem((2 * pairs, all_rows, LANES), f32),
            vmem((rad_len, 3 * rad_len), bf16),
            vmem((2 * lat_len, 2 * LANES), bf16),
            vmem((2 * lat_len, 2 * LANES), bf16),
            vmem((3 * LANES, lat_len), bf16),
            vmem((count, SUB, LANES), f32),
            vmem((1, LANES), f32),
            vmem((others, 1, LANES), f32),
            vmem((LANES, LANES), f32),
            vmem((LANES, LANES), f32),
            vmem((2 * pairs, LANES), f32),
            vmem((1, LANES), f32),
            vmem((others, 1, LANES), f32),
            pltpu.SemaphoreType.REGULAR((n_c // 2,)),
            dma((LOADS + 2,)),
            dma((2, LOADS)),
            dma((2, LOADS)),
            dma((part // SUB, 2)),
            dma((part // SUB, 2)),
            dma((part // SUB, 2)),
            dma((part // SUB, 2)),
            dma((others,)),
            dma((others,)),
            dma((others,)),
            dma((others,)),
        ],
        compiler_params=pltpu.CompilerParams(
            collective_id=0, has_side_effects=True, vmem_limit_bytes=61905306
        ),
    )(
        kernels.reshape(2, RIM, rad_len, lat_len),
        steps.reshape(pairs, all_rows, lat_len),
        curvature.reshape(pairs, all_rows, lat_len),
    )
    blocks = 4
    gradient, direction = pl.pallas_call(
        functools.partial(combine_kernel, pairs, blocks),
        out_shape=(out, out),
        in_specs=[vmem_spec] * 4,
        out_specs=(any_spec, any_spec),
        scratch_shapes=[vmem((all_rows, lat_len), f32), dma((blocks + 1,))],
        compiler_params=pltpu.CompilerParams(vmem_limit_bytes=2 * 1024 * 1024),
    )(*staged)
    shape = (lons, part, lat_len)
    return gradient.reshape(shape), direction.reshape(shape)


def solution(mesh):
    placed = (
        P("event", "cuts", None, None),
        P(None, "cuts", "event", None),
        P(None, "cuts", "event", None),
    )
    return jax.shard_map(
        shards,
        mesh=mesh,
        in_specs=placed,
        out_specs=(P("cuts", "event", None), P("cuts", "event", None)),
        check_vma=False,
    )
```

```python
import functools
import math

import jax
import jax.numpy as jnp
from jax import lax
from jax.experimental import pallas as pl
from jax.experimental.pallas import tpu as pltpu
from jax.sharding import PartitionSpec as P

RIM = 4
LOADS = 4
LANES = 128
SUB = 8
MESH = pl.DeviceIdType.MESH
HIGHEST = lax.Precision.HIGHEST


def cycle_weights():
    unscaled = [math.exp(-((column - RIM) ** 2) / 4.5) for column in range(2 * RIM + 1)]
    whole = sum(unscaled)
    return [weight / whole for weight in unscaled]


def halves(value):
    high = value.astype(jnp.bfloat16)
    return high, (value - high.astype(jnp.float32)).astype(jnp.bfloat16)


def unscaled_gauss(length, sigma):
    rows = lax.broadcasted_iota(jnp.int32, (length, length), 0)
    columns = lax.broadcasted_iota(jnp.int32, (length, length), 1)
    offset = (rows - columns).astype(jnp.float32)
    return jnp.exp(-offset * offset / (2.0 * sigma * sigma))


def factor(shape, spot_axis, length, sigma, count):
    reach = 2.25 * sigma
    pitch = (length - 1 + 2 * reach) / (count - 1)
    assert pitch < 0.54 * sigma
    spots = lax.broadcasted_iota(jnp.int32, shape, spot_axis).astype(jnp.float32)
    nodes = lax.broadcasted_iota(jnp.int32, shape, 1 - spot_axis).astype(jnp.float32)
    offset = spots - (nodes * pitch - reach)
    return jnp.exp(-offset * offset / (sigma * sigma))


def upper(pairs):
    return [(i, j) for i in range(pairs) for j in range(i, pairs)]


def kernel(
    sizes,
    kern_hbm, steps_hbm, curv_hbm, out,
    steps, changes, kern, rad, far_in, near_in, far_out, x_in, nodes, halo_in, smooth, short,
    rad_mat, pack_mat, dual_mat, lat_mat, gram_acc, gram_row, gram_all,
    table, splat, mix, late_row, late_all,
    ready, load_sem, core_send, core_recv, x_send, x_recv, halo_send, halo_recv,
    gram_send, gram_recv, late_send, late_recv,
):
    n_c, n_e, pairs, rad_len, lat_len = sizes
    grad, direc = out.at[0], out.at[1]
    part = rad_len // n_e
    c = lax.axis_index("cuts")
    e = lax.axis_index("event")
    barrier = pltpu.get_barrier_semaphore()
    steps_left, steps_right = c >= 2, c + 2 < n_c
    rounds = n_c // 2

    def flip(place):
        return c + place * (1 - 2 * lax.rem(c // place, 2))

    def greet(semaphore):
        for d in range(1, n_e):
            pl.semaphore_signal(
                semaphore, 1, device_id={"event": lax.rem(e + d, n_e)}, device_id_type=MESH
            )
        pl.semaphore_signal(semaphore, 1, device_id={"cuts": flip(1)}, device_id_type=MESH)

        @pl.when(steps_left)
        def _():
            pl.semaphore_signal(semaphore, 1, device_id={"cuts": c - 2}, device_id_type=MESH)

        @pl.when(steps_right)
        def _():
            pl.semaphore_signal(semaphore, 1, device_id={"cuts": c + 2}, device_id_type=MESH)

    def greeted(semaphore):
        pl.semaphore_wait(
            semaphore, n_e + steps_left.astype(jnp.int32) + steps_right.astype(jnp.int32)
        )

    def relay(number):
        greeted(ready.at[number - 1] if number else barrier)
        if number < rounds:
            greet(ready.at[number])

    greet(barrier)
    others = []
    for mask in reversed(range(n_c)):
        where = c
        for bit in range(mask.bit_length()):
            if mask >> bit & 1:
                where = where + (flip(1 << bit) - c)
        for d in range(n_e):
            if mask or d:
                others.append({"cuts": where, "event": lax.rem(e + d, n_e)})

    per = 2 * RIM // LOADS
    loads = []
    for p in range(LOADS):
        side, ks = p * per // RIM, pl.ds(p * per % RIM, per)
        loads.append(pltpu.make_async_copy(
            kern_hbm.at[side, ks], kern.at[side, ks], load_sem.at[p]
        ))
        loads[-1].start()
    loads.append(pltpu.make_async_copy(steps_hbm, steps, load_sem.at[LOADS]))
    loads.append(pltpu.make_async_copy(curv_hbm, changes, load_sem.at[LOADS + 1]))

    matrix = unscaled_gauss(rad_len, 3.0)
    high, low = halves(matrix / jnp.sum(matrix, axis=1, keepdims=True))
    rad_mat[...] = jnp.concatenate([high, high, low], axis=1)
    spread_out = factor((lat_len, LANES), 0, lat_len, 4.0, LANES)
    high, low = halves(spread_out)
    both = jnp.concatenate([high, low], axis=1)
    pack_mat[...] = jnp.concatenate([both, both], axis=0)
    table[...] = jnp.zeros_like(table)

    core = e + 1 - 2 * lax.rem(e, 2)
    far = lax.rem(e + 2, n_e)
    core_far = lax.rem(core + 2, n_e)

    def rows(chunk):
        return pl.ds(pl.multiple_of(chunk * part, part), part)

    def send(src, dst, send_sem, recv_sem, where):
        return pltpu.make_async_remote_copy(
            src_ref=src, dst_ref=dst, send_sem=send_sem, recv_sem=recv_sem,
            device_id=where, device_id_type=MESH,
        )

    far_copies, near_copies, x_copies, halo_copies = [], [], [], []

    def packed(value, matrix):
        high, low = halves(value)
        out = jnp.dot(
            jnp.concatenate([high, low], axis=1), matrix[...], preferred_element_type=jnp.float32
        )
        return out[:, :LANES] + out[:, LANES:]

    for p in range(LOADS):
        side, first = p * per // RIM, p * per % RIM
        loads[p].wait()
        if p == LOADS - 1:
            for load in loads[LOADS:]:
                load.start()
        value = packed(
            kern[side, pl.ds(first, per)].reshape(per * rad_len, lat_len), pack_mat
        ).reshape(per, rad_len, LANES)
        high, low = halves(jnp.concatenate([value[k] for k in range(per)], axis=1))
        value = jnp.dot(
            rad_mat[...], jnp.concatenate([high, low, high], axis=0),
            preferred_element_type=jnp.float32,
        )
        for k in range(per):
            rad[side, first + k] = value[:, k * LANES : (k + 1) * LANES]
    relay(0)
    for number, (copies, chunk, into) in enumerate(
        ((far_copies, core_far, far_in), (near_copies, core, near_in))
    ):
        for p in range(LOADS):
            side, ks = p * per // RIM, pl.ds(p * per % RIM, per)
            copies.append(send(
                rad.at[side, ks, rows(chunk)], into.at[side, ks],
                core_send.at[number, p], core_recv.at[number, p], {"event": core},
            ))
            copies[-1].start()
    strips = part // SUB
    sides = (lax.rem(c, 2), 1 - lax.rem(c, 2))
    pieces = [(h, turn) for turn in range(2) for h in range(strips)]

    def strip_rows(chunk, h):
        return pl.ds(pl.multiple_of(chunk * part + h * SUB, SUB), SUB)

    matrix = spread_out * jnp.sum(spread_out, axis=0, keepdims=True)
    high, low = halves(spread_out / jnp.sum(matrix, axis=1, keepdims=True))
    both = jnp.concatenate([high, low], axis=1)
    dual_mat[...] = jnp.concatenate([both, both], axis=0)
    matrix = factor((LANES, lat_len), 1, lat_len, 4.0, LANES)
    whole = jnp.sum(matrix * jnp.sum(matrix, axis=1, keepdims=True), axis=0, keepdims=True)
    high, low = halves(matrix / whole)
    lat_mat[...] = jnp.concatenate([high, high, low], axis=0)

    for copy in far_copies:
        copy.wait_recv()
    for h, turn in pieces:
        here, g = pl.ds(h * SUB, SUB), sides[turn]
        far_out[g, :, here] = rad[g, :, strip_rows(far, h)] + far_in[g, :, here]
        x_copies.append(send(
            far_out.at[g, :, here], x_in.at[g, :, here], x_send.at[h, turn], x_recv.at[h, turn],
            {"event": far},
        ))
        x_copies[-1].start()
    relay(1)

    slots = {pair: number for number, pair in enumerate(upper(pairs))}
    count = len(slots)
    groups = [(0, 1), (2, 3), tuple(range(4, pairs))]
    all_rows = steps.shape[1]
    tiles = all_rows // SUB
    lats = lat_len // LANES
    strip = tiles // RIM

    def gram(number):
        if number == 0:
            loads[LOADS].wait()
            loads[LOADS + 1].wait()

        def scale(t, _):
            place = pl.ds(pl.multiple_of(t * SUB, SUB), SUB)
            for i in range(pairs):
                changes[i, place, :] = changes[i, place, :] * steps[i, place, :]
            return 0

        lax.fori_loop(number * strip, (number + 1) * strip, scale, 0, unroll=2)
        for group in groups:
            wanted = [(i, j) for i in group for j in range(i, pairs)]

            def body(t, sums):
                place = pl.ds(pl.multiple_of(t * SUB, SUB), SUB)
                sums = list(sums)
                for lane in range(lats):
                    across = pl.ds(lane * LANES, LANES)
                    change = {j: changes[j, place, across] for j in range(group[0], pairs)}
                    for n, i in enumerate(group):
                        step = steps[i, place, across]
                        for m, (a, b) in enumerate(wanted):
                            if a == i:
                                sums[2 * m] = sums[2 * m] + step * change[b]
                                sums[2 * m + 1] = sums[2 * m + 1] + change[i] * change[b]
                return tuple(sums)

            sums = lax.fori_loop(
                number * strip, (number + 1) * strip, body,
                tuple(jnp.zeros((SUB, LANES), jnp.float32) for _ in range(2 * len(wanted))),
            )
            for m, pair in enumerate(wanted):
                for kind in range(2):
                    place = slots[pair] + kind * count
                    if number == 0:
                        gram_acc[place] = sums[2 * m + kind]
                    else:
                        gram_acc[place] = gram_acc[place] + sums[2 * m + kind]

    def spread(row, slot_refs, sends, recvs):
        for d, other in enumerate(others):
            send(row, slot_refs.at[d], sends.at[d], recvs.at[d], other).start()
        return [
            send(row, slot_refs.at[d], sends.at[d], recvs.at[d], other)
            for d, other in enumerate(others)
        ]

    def gathered(row, slot_refs, copies):
        for copy in copies:
            copy.wait_recv()
        return row[...] + jnp.sum(slot_refs[...], axis=0)

    def arrive(number):
        h, turn = pieces[number]
        here, g = pl.ds(h * SUB, SUB), sides[turn]
        base = rad[g, :, strip_rows(e, h)] + near_in[g, :, here]
        x_copies[number].wait_recv()
        nodes[g, :, here] = base + x_in[g, :, here]
        halo_copies.append(send(
            nodes.at[g, :, here], halo_in.at[g, :, here], halo_send.at[h, g], halo_recv.at[h, g],
            {"cuts": lax.rem(c + n_c - 1 + 2 * g, n_c)},
        ))
        halo_copies[-1].start()

    def shorten(kind, vector):
        for i in range(pairs):
            short[kind * pairs + i] = packed(vector[i], dual_mat)

    weights = cycle_weights()
    lons = 2 * RIM

    def finish(h):
        for copy in halo_copies[h::strips]:
            copy.wait_recv()
        place = pl.ds(h * SUB, SUB)
        padded = (
            [halo_in[1, k, place] for k in range(RIM)]
            + [nodes[side, k, place] for side in range(2) for k in range(RIM)]
            + [halo_in[0, k, place] for k in range(RIM)]
        )
        sums = [None] * (2 * pairs)
        for a in range(lons):
            value = weights[RIM] * padded[a + RIM]
            for k in range(1, RIM + 1):
                value = value + weights[RIM + k] * (padded[a + RIM - k] + padded[a + RIM + k])
            spot = pl.ds(a * part + h * SUB, SUB)
            smooth[spot, :] = value
            for n in range(2 * pairs):
                term = value * short[n, spot, :]
                sums[n] = term if sums[n] is None else sums[n] + term
        for n in range(2 * pairs):
            place = pl.ds(n * SUB, SUB)
            table[place, :] = sums[n] if h == 0 else table[place, :] + sums[n]

    gram(0)
    relay(2)
    shorten(0, steps)
    for number in range(3, rounds):
        relay(number)
    gram(1)
    for copy in near_copies:
        copy.wait_recv()
    for number in range(len(pieces)):
        arrive(number)
    relay(rounds)
    gram(2)
    gram(3)
    ones = jnp.ones((LANES, LANES), jnp.float32)

    def lane_sums(value):
        return lax.dot_general(
            ones[:SUB], value, (((1,), (1,)), ((), ())), precision=HIGHEST,
            preferred_element_type=jnp.float32,
        )[:1]

    table[pl.ds(0, 2 * count), :] = jnp.sum(gram_acc[...], axis=1)
    gram_row[...] = lane_sums(table[...])
    gram_copies = spread(gram_row, gram_all, gram_send, gram_recv)
    shorten(1, changes)
    for h in range(strips):
        finish(h)
    first, _ = halves(table[...])
    second, third = halves(table[...] - first.astype(jnp.float32))
    late_row[...] = lax.dot_general(
        jnp.ones((SUB, 3 * LANES), jnp.bfloat16), jnp.concatenate([first, second, third], axis=1),
        (((1,), (1,)), ((), ())), preferred_element_type=jnp.float32,
    )[:1]
    late_copies = spread(late_row, late_all, late_send, late_recv)
    high, low = halves(smooth[...])
    grad[...] = jnp.dot(
        jnp.concatenate([high, low, high], axis=1), lat_mat[...],
        preferred_element_type=jnp.float32,
    )
    products = gathered(gram_row, gram_all, gram_copies)
    square = (LANES, LANES)
    on_diagonal = lax.broadcasted_iota(jnp.int32, square, 0) == lax.broadcasted_iota(jnp.int32, square, 1)
    splat[...] = jnp.dot(
        jnp.where(on_diagonal, jnp.broadcast_to(products, square), 0.0), ones,
        precision=HIGHEST, preferred_element_type=jnp.float32,
    )

    def cross(i, j):
        place = slots[i, j]
        return splat[place : place + 1, :]

    def squared(i, j):
        place = count + slots[min(i, j), max(i, j)]
        return splat[place : place + 1, :]

    def unit(place):
        return (lax.broadcasted_iota(jnp.int32, (1, LANES), 1) // SUB == place).astype(jnp.float32)

    inverse = [1.0 / cross(i, i) for i in range(pairs)]
    scaling = cross(pairs - 1, pairs - 1) / squared(pairs - 1, pairs - 1)
    alphas = [None] * pairs
    for i in reversed(range(pairs)):
        row = unit(i)
        for j in range(pairs - 1, i, -1):
            row = row - cross(i, j) * alphas[j]
        alphas[i] = inverse[i] * row
    onto = []
    for i in range(pairs):
        row = unit(pairs + i)
        for j in range(pairs):
            row = row - squared(i, j) * alphas[j]
        row = scaling * row
        for j in range(i):
            row = row + cross(j, i) * onto[j]
        onto.append(alphas[i] - inverse[i] * row)
    for i in range(pairs):
        mix[i : i + 1, :] = -onto[i]
        mix[pairs + i : pairs + i + 1, :] = scaling * alphas[i]

    for copies in (far_copies, near_copies, x_copies, halo_copies, gram_copies, late_copies):
        for copy in copies:
            copy.wait_send()
    products = gathered(late_row, late_all, late_copies)
    mixed = jnp.sum(mix[...] * products, axis=1, keepdims=True)
    factors = [
        jnp.broadcast_to(mixed[i : i + 1], (SUB, LANES)) for i in range(2 * pairs)
    ]
    ratio = jnp.broadcast_to(-scaling, (SUB, LANES))

    def combine(t, _):
        place = pl.ds(pl.multiple_of(t * SUB, SUB), SUB)
        for lane in range(lats):
            across = pl.ds(lane * LANES, LANES)
            value = ratio * grad[place, across]
            for i in range(pairs):
                value = value + factors[i] * steps[i, place, across]
                value = value + factors[pairs + i] * changes[i, place, across]
            direc[place, across] = value
        return 0

    lax.fori_loop(0, tiles, combine, 0, unroll=4)


def shards(kernels, steps, curvature):
    n_c, n_e = lax.axis_size("cuts"), lax.axis_size("event")
    _, lons, rad_len, lat_len = kernels.shape
    pairs = steps.shape[0]
    part = rad_len // n_e
    assert lons == 2 * RIM and n_e == 4 and n_c % 2 == 0
    all_rows = lons * part
    count = pairs * (pairs + 1)
    f32, bf16 = jnp.float32, jnp.bfloat16
    vmem, dma = pltpu.VMEM, pltpu.SemaphoreType.DMA
    whole = (2, RIM, part, LANES)
    vmem_spec = pl.BlockSpec(memory_space=pltpu.VMEM)
    any_spec = pl.BlockSpec(memory_space=pl.ANY)
    others = n_c * n_e - 1
    assert 2 * pairs * SUB == LANES
    outs = pl.pallas_call(
        functools.partial(kernel, (n_c, n_e, pairs, rad_len, lat_len)),
        out_shape=vmem((2, all_rows, lat_len), f32),
        in_specs=[any_spec] * 3,
        out_specs=vmem_spec,
        scratch_shapes=[
            vmem((pairs, all_rows, lat_len), f32),
            vmem((pairs, all_rows, lat_len), f32),
            vmem((2, RIM, rad_len, lat_len), f32),
            vmem((2, RIM, rad_len, LANES), f32),
            vmem(whole, f32),
            vmem(whole, f32),
            vmem(whole, f32),
            vmem(whole, f32),
            vmem(whole, f32),
            vmem(whole, f32),
            vmem((all_rows, LANES), f32),
            vmem((2 * pairs, all_rows, LANES), f32),
            vmem((rad_len, 3 * rad_len), bf16),
            vmem((2 * lat_len, 2 * LANES), bf16),
            vmem((2 * lat_len, 2 * LANES), bf16),
            vmem((3 * LANES, lat_len), bf16),
            vmem((count, SUB, LANES), f32),
            vmem((1, LANES), f32),
            vmem((others, 1, LANES), f32),
            vmem((LANES, LANES), f32),
            vmem((LANES, LANES), f32),
            vmem((2 * pairs, LANES), f32),
            vmem((1, LANES), f32),
            vmem((others, 1, LANES), f32),
            pltpu.SemaphoreType.REGULAR((n_c // 2,)),
            dma((LOADS + 2,)),
            dma((2, LOADS)),
            dma((2, LOADS)),
            dma((part // SUB, 2)),
            dma((part // SUB, 2)),
            dma((part // SUB, 2)),
            dma((part // SUB, 2)),
            dma((others,)),
            dma((others,)),
            dma((others,)),
            dma((others,)),
        ],
        compiler_params=pltpu.CompilerParams(
            collective_id=0, has_side_effects=True, vmem_limit_bytes=61905306
        ),
    )(
        kernels.reshape(2, RIM, rad_len, lat_len),
        steps.reshape(pairs, all_rows, lat_len),
        curvature.reshape(pairs, all_rows, lat_len),
    )
    shape = (lons, part, lat_len)
    return outs[0].reshape(shape), outs[1].reshape(shape)


def solution(mesh):
    placed = (
        P("event", "cuts", None, None),
        P(None, "cuts", "event", None),
        P(None, "cuts", "event", None),
    )
    return jax.shard_map(
        shards,
        mesh=mesh,
        in_specs=placed,
        out_specs=(P("cuts", "event", None), P("cuts", "event", None)),
        check_vma=False,
    )
```

```python
import functools
import math

import jax
import jax.numpy as jnp
from jax import lax
from jax.experimental import pallas as pl
from jax.experimental.pallas import tpu as pltpu
from jax.sharding import PartitionSpec as P

RIM = 4
LOADS = 4
LANES = 128
SUB = 8
MESH = pl.DeviceIdType.MESH
HIGHEST = lax.Precision.HIGHEST


def cycle_weights():
    unscaled = [math.exp(-((column - RIM) ** 2) / 4.5) for column in range(2 * RIM + 1)]
    whole = sum(unscaled)
    return [weight / whole for weight in unscaled]


def halves(value):
    high = value.astype(jnp.bfloat16)
    return high, (value - high.astype(jnp.float32)).astype(jnp.bfloat16)


def unscaled_gauss(length, sigma):
    rows = lax.broadcasted_iota(jnp.int32, (length, length), 0)
    columns = lax.broadcasted_iota(jnp.int32, (length, length), 1)
    offset = (rows - columns).astype(jnp.float32)
    return jnp.exp(-offset * offset / (2.0 * sigma * sigma))


def factor(shape, spot_axis, length, sigma, count):
    reach = 2.25 * sigma
    pitch = (length - 1 + 2 * reach) / (count - 1)
    assert pitch < 0.54 * sigma
    spots = lax.broadcasted_iota(jnp.int32, shape, spot_axis).astype(jnp.float32)
    nodes = lax.broadcasted_iota(jnp.int32, shape, 1 - spot_axis).astype(jnp.float32)
    offset = spots - (nodes * pitch - reach)
    return jnp.exp(-offset * offset / (sigma * sigma))


def upper(pairs):
    return [(i, j) for i in range(pairs) for j in range(i, pairs)]


def kernel(
    sizes,
    kern_hbm, steps_hbm, curv_hbm, out,
    steps, changes, kern, rad, far_in, near_in, far_out, x_in, nodes, halo_in, smooth, short,
    rad_mat, pack_mat, dual_mat, lat_mat, gram_acc, gram_row, gram_all,
    table, splat, mix, late_row, late_all,
    ready, load_sem, core_send, core_recv, x_send, x_recv, halo_send, halo_recv,
    gram_send, gram_recv, late_send, late_recv,
):
    n_c, n_e, pairs, rad_len, lat_len = sizes
    grad, direc = out.at[0], out.at[1]
    part = rad_len // n_e
    c = lax.axis_index("cuts")
    e = lax.axis_index("event")
    barrier = pltpu.get_barrier_semaphore()
    steps_left, steps_right = c >= 2, c + 2 < n_c

    def flip(place):
        return c + place * (1 - 2 * lax.rem(c // place, 2))

    def signal(semaphore, **where):
        pl.semaphore_signal(semaphore, 1, device_id=where, device_id_type=MESH)

    for d in range(1, n_e):
        signal(barrier, event=lax.rem(e + d, n_e))
    signal(barrier, cuts=flip(1))

    @pl.when(steps_left)
    def _():
        signal(barrier, cuts=c - 2)

    @pl.when(steps_right)
    def _():
        signal(barrier, cuts=c + 2)

    def enter():
        pl.semaphore_wait(barrier, n_e + steps_left.astype(jnp.int32) + steps_right.astype(jnp.int32))

        @pl.when(jnp.logical_not(steps_left) & steps_right)
        def _():
            signal(ready.at[0], cuts=c + 2)

        @pl.when(jnp.logical_not(steps_right) & steps_left)
        def _():
            signal(ready.at[1], cuts=c - 2)

    def pass_right():
        @pl.when(steps_left)
        def _():
            pl.semaphore_wait(ready.at[0], 1)

            @pl.when(steps_right)
            def _():
                signal(ready.at[0], cuts=c + 2)

    def pass_left():
        @pl.when(steps_left)
        def _():
            @pl.when(steps_right)
            def _():
                pl.semaphore_wait(ready.at[1], 1)
                signal(ready.at[1], cuts=c - 2)

            signal(ready.at[2], cuts=flip(1))

    def end_left():
        @pl.when(jnp.logical_not(steps_left))
        def _():
            @pl.when(steps_right)
            def _():
                pl.semaphore_wait(ready.at[1], 1)

            signal(ready.at[2], cuts=flip(1))

    others = []
    for mask in reversed(range(n_c)):
        where = c
        for bit in range(mask.bit_length()):
            if mask >> bit & 1:
                where = where + (flip(1 << bit) - c)
        for d in range(n_e):
            if mask or d:
                others.append({"cuts": where, "event": lax.rem(e + d, n_e)})

    sides = (lax.rem(c, 2), 1 - lax.rem(c, 2))
    per = 2 * RIM // LOADS
    chunks = [(sides[p * per // RIM], p * per % RIM) for p in range(LOADS)]
    loads = []
    for p, (g, first) in enumerate(chunks):
        ks = pl.ds(first, per)
        loads.append(pltpu.make_async_copy(kern_hbm.at[g, ks], kern.at[g, ks], load_sem.at[p]))
        loads[-1].start()
    loads.append(pltpu.make_async_copy(steps_hbm, steps, load_sem.at[LOADS]))
    loads.append(pltpu.make_async_copy(curv_hbm, changes, load_sem.at[LOADS + 1]))

    matrix = unscaled_gauss(rad_len, 3.0)
    high, low = halves(matrix / jnp.sum(matrix, axis=1, keepdims=True))
    rad_mat[...] = jnp.concatenate([high, high, low], axis=1)
    spread_out = factor((lat_len, LANES), 0, lat_len, 4.0, LANES)
    high, low = halves(spread_out)
    both = jnp.concatenate([high, low], axis=1)
    pack_mat[...] = jnp.concatenate([both, both], axis=0)
    table[...] = jnp.zeros_like(table)

    core = e + 1 - 2 * lax.rem(e, 2)
    far = lax.rem(e + 2, n_e)
    core_far = lax.rem(core + 2, n_e)

    def rows(chunk):
        return pl.ds(pl.multiple_of(chunk * part, part), part)

    def send(src, dst, send_sem, recv_sem, where):
        return pltpu.make_async_remote_copy(
            src_ref=src, dst_ref=dst, send_sem=send_sem, recv_sem=recv_sem,
            device_id=where, device_id_type=MESH,
        )

    far_copies, near_copies, x_copies, halo_copies = [], [], [], []

    def packed(value, matrix):
        high, low = halves(value)
        out = jnp.dot(
            jnp.concatenate([high, low], axis=1), matrix[...], preferred_element_type=jnp.float32
        )
        return out[:, :LANES] + out[:, LANES:]

    def exchange(p):
        g, first = chunks[p]
        ks = pl.ds(first, per)
        for number, (copies, chunk, into) in enumerate(
            ((far_copies, core_far, far_in), (near_copies, core, near_in))
        ):
            copies.append(send(
                rad.at[g, ks, rows(chunk)], into.at[g, ks],
                core_send.at[number, p], core_recv.at[number, p], {"event": core},
            ))
            copies[-1].start()

    value = None
    for p in range(LOADS + 1):
        before = value
        if p < LOADS:
            g, first = chunks[p]
            loads[p].wait()
            if p == LOADS - 1:
                for load in loads[LOADS:]:
                    load.start()
            value = packed(
                kern[g, pl.ds(first, per)].reshape(per * rad_len, lat_len), pack_mat
            ).reshape(per, rad_len, LANES)
        if p:
            high, low = halves(jnp.concatenate([before[k] for k in range(per)], axis=1))
            done = jnp.dot(
                rad_mat[...], jnp.concatenate([high, low, high], axis=0),
                preferred_element_type=jnp.float32,
            )
            g, first = chunks[p - 1]
            for k in range(per):
                rad[g, first + k] = done[:, k * LANES : (k + 1) * LANES]
            if p == 2:
                enter()
                exchange(0)
            if p >= 2:
                exchange(p - 1)
    strips = part // SUB

    matrix = spread_out * jnp.sum(spread_out, axis=0, keepdims=True)
    high, low = halves(spread_out / jnp.sum(matrix, axis=1, keepdims=True))
    both = jnp.concatenate([high, low], axis=1)
    dual_mat[...] = jnp.concatenate([both, both], axis=0)
    matrix = factor((LANES, lat_len), 1, lat_len, 4.0, LANES)
    whole = jnp.sum(matrix * jnp.sum(matrix, axis=1, keepdims=True), axis=0, keepdims=True)
    high, low = halves(matrix / whole)
    lat_mat[...] = jnp.concatenate([high, high, low], axis=0)

    for p, (g, first) in enumerate(chunks):
        ks = pl.ds(first, per)
        far_copies[p].wait_recv()
        far_out[g, ks] = rad[g, ks, rows(far)] + far_in[g, ks]
        x_copies.append(send(
            far_out.at[g, ks], x_in.at[g, ks], x_send.at[p], x_recv.at[p], {"event": far}
        ))
        x_copies[-1].start()
    pass_right()

    slots = {pair: number for number, pair in enumerate(upper(pairs))}
    count = len(slots)
    groups = [(0, 1), (2, 3), tuple(range(4, pairs))]
    all_rows = steps.shape[1]
    tiles = all_rows // SUB
    lats = lat_len // LANES
    strip = tiles // RIM

    def gram(number):
        if number == 0:
            loads[LOADS].wait()
            loads[LOADS + 1].wait()

        def scale(t, _):
            place = pl.ds(pl.multiple_of(t * SUB, SUB), SUB)
            for i in range(pairs):
                changes[i, place, :] = changes[i, place, :] * steps[i, place, :]
            return 0

        lax.fori_loop(number * strip, (number + 1) * strip, scale, 0, unroll=2)
        for group in groups:
            wanted = [(i, j) for i in group for j in range(i, pairs)]

            def body(t, sums):
                place = pl.ds(pl.multiple_of(t * SUB, SUB), SUB)
                sums = list(sums)
                for lane in range(lats):
                    across = pl.ds(lane * LANES, LANES)
                    change = {j: changes[j, place, across] for j in range(group[0], pairs)}
                    for n, i in enumerate(group):
                        step = steps[i, place, across]
                        for m, (a, b) in enumerate(wanted):
                            if a == i:
                                sums[2 * m] = sums[2 * m] + step * change[b]
                                sums[2 * m + 1] = sums[2 * m + 1] + change[i] * change[b]
                return tuple(sums)

            sums = lax.fori_loop(
                number * strip, (number + 1) * strip, body,
                tuple(jnp.zeros((SUB, LANES), jnp.float32) for _ in range(2 * len(wanted))),
            )
            for m, pair in enumerate(wanted):
                for kind in range(2):
                    place = slots[pair] + kind * count
                    if number == 0:
                        gram_acc[place] = sums[2 * m + kind]
                    else:
                        gram_acc[place] = gram_acc[place] + sums[2 * m + kind]

    def spread(row, slot_refs, sends, recvs):
        for d, other in enumerate(others):
            send(row, slot_refs.at[d], sends.at[d], recvs.at[d], other).start()
        return [
            send(row, slot_refs.at[d], sends.at[d], recvs.at[d], other)
            for d, other in enumerate(others)
        ]

    def gathered(row, slot_refs, copies):
        for copy in copies:
            copy.wait_recv()
        return row[...] + jnp.sum(slot_refs[...], axis=0)

    def arrive(p):
        g, first = chunks[p]
        ks = pl.ds(first, per)
        near_copies[p].wait_recv()
        base = rad[g, ks, rows(e)] + near_in[g, ks]
        x_copies[p].wait_recv()
        nodes[g, ks] = base + x_in[g, ks]
        halo_copies.append(send(
            nodes.at[g, ks], halo_in.at[g, ks], halo_send.at[p], halo_recv.at[g, first // per],
            {"cuts": lax.rem(c + n_c - 1 + 2 * g, n_c)},
        ))
        halo_copies[-1].start()

    def shorten(kind, vector, first, last):
        for i in range(first, last):
            short[kind * pairs + i] = packed(vector[i], dual_mat)

    weights = cycle_weights()

    def finish(turn):
        g = sides[turn]
        for p in range(turn * LOADS // 2, (turn + 1) * LOADS // 2):
            first = chunks[p][1]
            ks = pl.ds(first, per)
            send(
                nodes.at[1 - g, ks], halo_in.at[1 - g, ks], halo_send.at[p],
                halo_recv.at[1 - g, first // per], {"event": core},
            ).wait_recv()

        def at(k):
            return k + g * (RIM - 1 - 2 * k)

        sums = [None] * (2 * pairs)
        for h in range(strips):
            place = pl.ds(h * SUB, SUB)
            padded = (
                [halo_in[1 - g, at(k), place] for k in range(RIM)]
                + [nodes[g, at(k), place] for k in range(RIM)]
                + [nodes[1 - g, at(k), place] for k in range(RIM)]
            )
            for a in range(RIM):
                value = weights[RIM] * padded[a + RIM]
                for k in range(1, RIM + 1):
                    value = value + weights[RIM + k] * (padded[a + RIM - k] + padded[a + RIM + k])
                spot = pl.ds(pl.multiple_of((g * RIM + at(a)) * part + h * SUB, SUB), SUB)
                smooth[spot, :] = value
                for n in range(2 * pairs):
                    term = value * short[n, spot, :]
                    sums[n] = term if sums[n] is None else sums[n] + term
        for n in range(2 * pairs):
            place = pl.ds(n * SUB, SUB)
            table[place, :] = sums[n] if turn == 0 else table[place, :] + sums[n]

    pass_left()
    for number in range(RIM):
        gram(number)
    end_left()
    ones = jnp.ones((LANES, LANES), jnp.float32)

    def lane_sums(value):
        return lax.dot_general(
            ones[:SUB], value, (((1,), (1,)), ((), ())), precision=HIGHEST,
            preferred_element_type=jnp.float32,
        )[:1]

    table[pl.ds(0, 2 * count), :] = jnp.sum(gram_acc[...], axis=1)
    gram_row[...] = lane_sums(table[...])
    for p in range(LOADS):
        arrive(p)
        shorten(0, steps, p * pairs // LOADS, (p + 1) * pairs // LOADS)
    pl.semaphore_wait(ready.at[2], 1)
    gram_copies = spread(gram_row, gram_all, gram_send, gram_recv)
    shorten(1, changes, 0, pairs)
    finish(0)
    finish(1)
    first, _ = halves(table[...])
    second, third = halves(table[...] - first.astype(jnp.float32))
    late_row[...] = lax.dot_general(
        jnp.ones((SUB, 3 * LANES), jnp.bfloat16), jnp.concatenate([first, second, third], axis=1),
        (((1,), (1,)), ((), ())), preferred_element_type=jnp.float32,
    )[:1]
    late_copies = spread(late_row, late_all, late_send, late_recv)
    high, low = halves(smooth[...])
    grad[...] = jnp.dot(
        jnp.concatenate([high, low, high], axis=1), lat_mat[...],
        preferred_element_type=jnp.float32,
    )
    products = gathered(gram_row, gram_all, gram_copies)
    square = (LANES, LANES)
    on_diagonal = lax.broadcasted_iota(jnp.int32, square, 0) == lax.broadcasted_iota(jnp.int32, square, 1)
    splat[...] = jnp.dot(
        jnp.where(on_diagonal, jnp.broadcast_to(products, square), 0.0), ones,
        precision=HIGHEST, preferred_element_type=jnp.float32,
    )

    def cross(i, j):
        place = slots[i, j]
        return splat[place : place + 1, :]

    def squared(i, j):
        place = count + slots[min(i, j), max(i, j)]
        return splat[place : place + 1, :]

    def unit(place):
        return (lax.broadcasted_iota(jnp.int32, (1, LANES), 1) // SUB == place).astype(jnp.float32)

    inverse = [1.0 / cross(i, i) for i in range(pairs)]
    scaling = cross(pairs - 1, pairs - 1) / squared(pairs - 1, pairs - 1)
    alphas = [None] * pairs
    for i in reversed(range(pairs)):
        row = unit(i)
        for j in range(pairs - 1, i, -1):
            row = row - cross(i, j) * alphas[j]
        alphas[i] = inverse[i] * row
    onto = []
    for i in range(pairs):
        row = unit(pairs + i)
        for j in range(pairs):
            row = row - squared(i, j) * alphas[j]
        row = scaling * row
        for j in range(i):
            row = row + cross(j, i) * onto[j]
        onto.append(alphas[i] - inverse[i] * row)
    for i in range(pairs):
        mix[i : i + 1, :] = -onto[i]
        mix[pairs + i : pairs + i + 1, :] = scaling * alphas[i]

    for copies in (far_copies, near_copies, x_copies, halo_copies, gram_copies, late_copies):
        for copy in copies:
            copy.wait_send()
    products = gathered(late_row, late_all, late_copies)
    mixed = jnp.sum(mix[...] * products, axis=1, keepdims=True)
    factors = [
        jnp.broadcast_to(mixed[i : i + 1], (SUB, LANES)) for i in range(2 * pairs)
    ]
    ratio = jnp.broadcast_to(-scaling, (SUB, LANES))

    def combine(t, _):
        place = pl.ds(pl.multiple_of(t * SUB, SUB), SUB)
        for lane in range(lats):
            across = pl.ds(lane * LANES, LANES)
            values = [ratio * grad[place, across]]
            for i in range(pairs):
                values.append(factors[i] * steps[i, place, across])
                values.append(factors[pairs + i] * changes[i, place, across])
            while len(values) > 1:
                paired = [x + y for x, y in zip(values[::2], values[1::2])]
                values = paired + values[2 * len(paired) :]
            direc[place, across] = values[0]
        return 0

    lax.fori_loop(0, tiles, combine, 0, unroll=4)


def shards(kernels, steps, curvature):
    n_c, n_e = lax.axis_size("cuts"), lax.axis_size("event")
    _, lons, rad_len, lat_len = kernels.shape
    pairs = steps.shape[0]
    part = rad_len // n_e
    assert lons == 2 * RIM and n_e == 4 and n_c % 2 == 0
    all_rows = lons * part
    count = pairs * (pairs + 1)
    f32, bf16 = jnp.float32, jnp.bfloat16
    vmem, dma = pltpu.VMEM, pltpu.SemaphoreType.DMA
    whole = (2, RIM, part, LANES)
    vmem_spec = pl.BlockSpec(memory_space=pltpu.VMEM)
    any_spec = pl.BlockSpec(memory_space=pl.ANY)
    others = n_c * n_e - 1
    assert 2 * pairs * SUB == LANES
    outs = pl.pallas_call(
        functools.partial(kernel, (n_c, n_e, pairs, rad_len, lat_len)),
        out_shape=vmem((2, all_rows, lat_len), f32),
        in_specs=[any_spec] * 3,
        out_specs=vmem_spec,
        scratch_shapes=[
            vmem((pairs, all_rows, lat_len), f32),
            vmem((pairs, all_rows, lat_len), f32),
            vmem((2, RIM, rad_len, lat_len), f32),
            vmem((2, RIM, rad_len, LANES), f32),
            vmem(whole, f32),
            vmem(whole, f32),
            vmem(whole, f32),
            vmem(whole, f32),
            vmem(whole, f32),
            vmem(whole, f32),
            vmem((all_rows, LANES), f32),
            vmem((2 * pairs, all_rows, LANES), f32),
            vmem((rad_len, 3 * rad_len), bf16),
            vmem((2 * lat_len, 2 * LANES), bf16),
            vmem((2 * lat_len, 2 * LANES), bf16),
            vmem((3 * LANES, lat_len), bf16),
            vmem((count, SUB, LANES), f32),
            vmem((1, LANES), f32),
            vmem((others, 1, LANES), f32),
            vmem((LANES, LANES), f32),
            vmem((LANES, LANES), f32),
            vmem((2 * pairs, LANES), f32),
            vmem((1, LANES), f32),
            vmem((others, 1, LANES), f32),
            pltpu.SemaphoreType.REGULAR((3,)),
            dma((LOADS + 2,)),
            dma((2, LOADS)),
            dma((2, LOADS)),
            dma((LOADS,)),
            dma((LOADS,)),
            dma((LOADS,)),
            dma((2, LOADS // 2)),
            dma((others,)),
            dma((others,)),
            dma((others,)),
            dma((others,)),
        ],
        compiler_params=pltpu.CompilerParams(
            collective_id=0, has_side_effects=True, vmem_limit_bytes=61905306
        ),
    )(
        kernels.reshape(2, RIM, rad_len, lat_len),
        steps.reshape(pairs, all_rows, lat_len),
        curvature.reshape(pairs, all_rows, lat_len),
    )
    shape = (lons, part, lat_len)
    return outs[0].reshape(shape), outs[1].reshape(shape)


def solution(mesh):
    placed = (
        P("event", "cuts", None, None),
        P(None, "cuts", "event", None),
        P(None, "cuts", "event", None),
    )
    return jax.shard_map(
        shards,
        mesh=mesh,
        in_specs=placed,
        out_specs=(P("cuts", "event", None), P("cuts", "event", None)),
        check_vma=False,
    )
```

```python
import functools
import math

import jax
import jax.numpy as jnp
from jax import lax
from jax.experimental import pallas as pl
from jax.experimental.pallas import tpu as pltpu
from jax.sharding import PartitionSpec as P

RIM = 4
LOADS = 4
LANES = 128
SUB = 8
MESH = pl.DeviceIdType.MESH
HIGHEST = lax.Precision.HIGHEST


def cycle_weights():
    unscaled = [math.exp(-((column - RIM) ** 2) / 4.5) for column in range(2 * RIM + 1)]
    whole = sum(unscaled)
    return [weight / whole for weight in unscaled]


def halves(value):
    high = value.astype(jnp.bfloat16)
    return high, (value - high.astype(jnp.float32)).astype(jnp.bfloat16)


def unscaled_gauss(length, sigma):
    rows = lax.broadcasted_iota(jnp.int32, (length, length), 0)
    columns = lax.broadcasted_iota(jnp.int32, (length, length), 1)
    offset = (rows - columns).astype(jnp.float32)
    return jnp.exp(-offset * offset / (2.0 * sigma * sigma))


def factor(shape, spot_axis, length, sigma, count):
    reach = 2.25 * sigma
    pitch = (length - 1 + 2 * reach) / (count - 1)
    assert pitch < 0.54 * sigma
    spots = lax.broadcasted_iota(jnp.int32, shape, spot_axis).astype(jnp.float32)
    nodes = lax.broadcasted_iota(jnp.int32, shape, 1 - spot_axis).astype(jnp.float32)
    offset = spots - (nodes * pitch - reach)
    return jnp.exp(-offset * offset / (sigma * sigma))


def upper(pairs):
    return [(i, j) for i in range(pairs) for j in range(i, pairs)]


def kernel(
    sizes,
    kern_hbm, steps_hbm, curv_hbm, out,
    steps, changes, kern, rad, far_in, near_in, far_out, x_in, cross_in, nodes, halo_in, smooth, short,
    rad_mat, pack_mat, dual_mat, lat_mat, gram_acc, gram_row, gram_all,
    table, splat, mix, late_row, late_all,
    ready, load_sem, core_send, core_recv, x_send, x_recv, halo_send, halo_recv,
    gram_send, gram_recv, late_send, late_recv,
):
    n_c, n_e, pairs, rad_len, lat_len = sizes
    grad, direc = out.at[0], out.at[1]
    part = rad_len // n_e
    c = lax.axis_index("cuts")
    e = lax.axis_index("event")
    barrier = pltpu.get_barrier_semaphore()
    steps_left, steps_right = c >= 2, c + 2 < n_c

    def flip(place):
        return c + place * (1 - 2 * lax.rem(c // place, 2))

    def signal(semaphore, **where):
        pl.semaphore_signal(semaphore, 1, device_id=where, device_id_type=MESH)

    for d in range(1, n_e):
        signal(barrier, event=lax.rem(e + d, n_e))
    signal(barrier, cuts=flip(1))

    @pl.when(steps_left)
    def _():
        signal(barrier, cuts=c - 2)

    @pl.when(steps_right)
    def _():
        signal(barrier, cuts=c + 2)

    def enter():
        pl.semaphore_wait(barrier, n_e + steps_left.astype(jnp.int32) + steps_right.astype(jnp.int32))

        @pl.when(jnp.logical_not(steps_left) & steps_right)
        def _():
            signal(ready.at[0], cuts=c + 2)

        @pl.when(jnp.logical_not(steps_right) & steps_left)
        def _():
            signal(ready.at[1], cuts=c - 2)

    def pass_right():
        @pl.when(steps_left)
        def _():
            pl.semaphore_wait(ready.at[0], 1)

            @pl.when(steps_right)
            def _():
                signal(ready.at[0], cuts=c + 2)

    def pass_left():
        @pl.when(steps_left)
        def _():
            @pl.when(steps_right)
            def _():
                pl.semaphore_wait(ready.at[1], 1)
                signal(ready.at[1], cuts=c - 2)

            signal(ready.at[2], cuts=flip(1))

    def end_left():
        @pl.when(jnp.logical_not(steps_left))
        def _():
            @pl.when(steps_right)
            def _():
                pl.semaphore_wait(ready.at[1], 1)

            signal(ready.at[2], cuts=flip(1))

    others = []
    for mask in reversed(range(n_c)):
        where = c
        for bit in range(mask.bit_length()):
            if mask >> bit & 1:
                where = where + (flip(1 << bit) - c)
        for d in range(n_e):
            if mask or d:
                others.append({"cuts": where, "event": lax.rem(e + d, n_e)})

    sides = (lax.rem(c, 2), 1 - lax.rem(c, 2))
    per = 2 * RIM // LOADS
    chunks = [(sides[p * per // RIM], p * per % RIM) for p in range(LOADS)]
    loads = []
    for p, (g, first) in enumerate(chunks):
        ks = pl.ds(first, per)
        loads.append(pltpu.make_async_copy(kern_hbm.at[g, ks], kern.at[g, ks], load_sem.at[p]))
        loads[-1].start()
    loads.append(pltpu.make_async_copy(steps_hbm, steps, load_sem.at[LOADS]))
    loads.append(pltpu.make_async_copy(curv_hbm, changes, load_sem.at[LOADS + 1]))

    matrix = unscaled_gauss(rad_len, 3.0)
    high, low = halves(matrix / jnp.sum(matrix, axis=1, keepdims=True))
    rad_mat[...] = jnp.concatenate([high, high, low], axis=1)
    spread_out = factor((lat_len, LANES), 0, lat_len, 4.0, LANES)
    high, low = halves(spread_out)
    both = jnp.concatenate([high, low], axis=1)
    pack_mat[...] = jnp.concatenate([both, both], axis=0)
    table[...] = jnp.zeros_like(table)

    core = e + 1 - 2 * lax.rem(e, 2)
    far = lax.rem(e + 2, n_e)
    core_far = lax.rem(core + 2, n_e)

    def rows(chunk):
        return pl.ds(pl.multiple_of(chunk * part, part), part)

    def send(src, dst, send_sem, recv_sem, where):
        return pltpu.make_async_remote_copy(
            src_ref=src, dst_ref=dst, send_sem=send_sem, recv_sem=recv_sem,
            device_id=where, device_id_type=MESH,
        )

    far_copies, near_copies, x_copies, halo_copies = [], [], [], []

    def packed(value, matrix):
        high, low = halves(value)
        out = jnp.dot(
            jnp.concatenate([high, low], axis=1), matrix[...], preferred_element_type=jnp.float32
        )
        return out[:, :LANES] + out[:, LANES:]

    def exchange(p):
        g, first = chunks[p]
        ks = pl.ds(first, per)
        if p == 0:
            for number, (where, into) in enumerate(((far, x_in.at[g, ks]), (core_far, cross_in))):
                x_copies.append(send(
                    rad.at[g, ks, rows(where)], into, x_send.at[number], x_recv.at[number],
                    {"event": where},
                ))
                x_copies[-1].start()
        for number, (copies, chunk, into) in enumerate(
            ((far_copies, core_far, far_in), (near_copies, core, near_in))
        ):
            if p or number:
                copies.append(send(
                    rad.at[g, ks, rows(chunk)], into.at[g, ks],
                    core_send.at[number, p], core_recv.at[number, p], {"event": core},
                ))
                copies[-1].start()

    value = None
    for p in range(LOADS + 1):
        before = value
        if p < LOADS:
            g, first = chunks[p]
            loads[p].wait()
            if p == LOADS - 1:
                for load in loads[LOADS:]:
                    load.start()
            value = packed(
                kern[g, pl.ds(first, per)].reshape(per * rad_len, lat_len), pack_mat
            ).reshape(per, rad_len, LANES)
        if p:
            high, low = halves(jnp.concatenate([before[k] for k in range(per)], axis=1))
            done = jnp.dot(
                rad_mat[...], jnp.concatenate([high, low, high], axis=0),
                preferred_element_type=jnp.float32,
            )
            g, first = chunks[p - 1]
            for k in range(per):
                rad[g, first + k] = done[:, k * LANES : (k + 1) * LANES]
            if p == 1:
                enter()
            exchange(p - 1)
    strips = part // SUB

    matrix = spread_out * jnp.sum(spread_out, axis=0, keepdims=True)
    high, low = halves(spread_out / jnp.sum(matrix, axis=1, keepdims=True))
    both = jnp.concatenate([high, low], axis=1)
    dual_mat[...] = jnp.concatenate([both, both], axis=0)
    matrix = factor((LANES, lat_len), 1, lat_len, 4.0, LANES)
    whole = jnp.sum(matrix * jnp.sum(matrix, axis=1, keepdims=True), axis=0, keepdims=True)
    high, low = halves(matrix / whole)
    lat_mat[...] = jnp.concatenate([high, high, low], axis=0)

    for copy, p in zip(far_copies, range(1, LOADS)):
        g, first = chunks[p]
        ks = pl.ds(first, per)
        copy.wait_recv()
        far_out[g, ks] = rad[g, ks, rows(far)] + far_in[g, ks]
        x_copies.append(send(
            far_out.at[g, ks], x_in.at[g, ks], x_send.at[p + 1], x_recv.at[p + 1],
            {"event": far},
        ))
        x_copies[-1].start()
    pass_right()

    slots = {pair: number for number, pair in enumerate(upper(pairs))}
    count = len(slots)
    groups = [(0, 1), (2, 3), tuple(range(4, pairs))]
    all_rows = steps.shape[1]
    tiles = all_rows // SUB
    lats = lat_len // LANES
    strip = tiles // RIM

    def gram(number):
        if number == 0:
            loads[LOADS].wait()
            loads[LOADS + 1].wait()

        def scale(t, _):
            place = pl.ds(pl.multiple_of(t * SUB, SUB), SUB)
            for i in range(pairs):
                changes[i, place, :] = changes[i, place, :] * steps[i, place, :]
            return 0

        lax.fori_loop(number * strip, (number + 1) * strip, scale, 0, unroll=2)
        for group in groups:
            wanted = [(i, j) for i in group for j in range(i, pairs)]

            def body(t, sums):
                place = pl.ds(pl.multiple_of(t * SUB, SUB), SUB)
                sums = list(sums)
                for lane in range(lats):
                    across = pl.ds(lane * LANES, LANES)
                    change = {j: changes[j, place, across] for j in range(group[0], pairs)}
                    for n, i in enumerate(group):
                        step = steps[i, place, across]
                        for m, (a, b) in enumerate(wanted):
                            if a == i:
                                sums[2 * m] = sums[2 * m] + step * change[b]
                                sums[2 * m + 1] = sums[2 * m + 1] + change[i] * change[b]
                return tuple(sums)

            sums = lax.fori_loop(
                number * strip, (number + 1) * strip, body,
                tuple(jnp.zeros((SUB, LANES), jnp.float32) for _ in range(2 * len(wanted))),
            )
            for m, pair in enumerate(wanted):
                for kind in range(2):
                    place = slots[pair] + kind * count
                    if number == 0:
                        gram_acc[place] = sums[2 * m + kind]
                    else:
                        gram_acc[place] = gram_acc[place] + sums[2 * m + kind]

    def spread(row, slot_refs, sends, recvs):
        for d, other in enumerate(others):
            send(row, slot_refs.at[d], sends.at[d], recvs.at[d], other).start()
        return [
            send(row, slot_refs.at[d], sends.at[d], recvs.at[d], other)
            for d, other in enumerate(others)
        ]

    def gathered(row, slot_refs, copies):
        for copy in copies:
            copy.wait_recv()
        return row[...] + jnp.sum(slot_refs[...], axis=0)

    def arrive(p):
        g, first = chunks[p]
        ks = pl.ds(first, per)
        near_copies[p].wait_recv()
        base = rad[g, ks, rows(e)] + near_in[g, ks]
        if p == 0:
            x_copies[0].wait_recv()
            x_copies[1].wait_recv()
            base = base + cross_in[...]
        else:
            x_copies[p + 1].wait_recv()
        nodes[g, ks] = base + x_in[g, ks]
        halo_copies.append(send(
            nodes.at[g, ks], halo_in.at[g, ks], halo_send.at[p], halo_recv.at[g, first // per],
            {"cuts": lax.rem(c + n_c - 1 + 2 * g, n_c)},
        ))
        halo_copies[-1].start()

    def shorten(kind, vector, first, last):
        for i in range(first, last):
            short[kind * pairs + i] = packed(vector[i], dual_mat)

    weights = cycle_weights()

    def finish(turn):
        g = sides[turn]
        for p in range(turn * LOADS // 2, (turn + 1) * LOADS // 2):
            first = chunks[p][1]
            ks = pl.ds(first, per)
            send(
                nodes.at[1 - g, ks], halo_in.at[1 - g, ks], halo_send.at[p],
                halo_recv.at[1 - g, first // per], {"event": core},
            ).wait_recv()

        def at(k):
            return k + g * (RIM - 1 - 2 * k)

        sums = [None] * (2 * pairs)
        for h in range(strips):
            place = pl.ds(h * SUB, SUB)
            padded = (
                [halo_in[1 - g, at(k), place] for k in range(RIM)]
                + [nodes[g, at(k), place] for k in range(RIM)]
                + [nodes[1 - g, at(k), place] for k in range(RIM)]
            )
            for a in range(RIM):
                value = weights[RIM] * padded[a + RIM]
                for k in range(1, RIM + 1):
                    value = value + weights[RIM + k] * (padded[a + RIM - k] + padded[a + RIM + k])
                spot = pl.ds(pl.multiple_of((g * RIM + at(a)) * part + h * SUB, SUB), SUB)
                smooth[spot, :] = value
                for n in range(2 * pairs):
                    term = value * short[n, spot, :]
                    sums[n] = term if sums[n] is None else sums[n] + term
        for n in range(2 * pairs):
            place = pl.ds(n * SUB, SUB)
            table[place, :] = sums[n] if turn == 0 else table[place, :] + sums[n]

    pass_left()
    gram(0)
    gram(1)
    end_left()
    for p in range(LOADS):
        arrive(p)
        if p < 2:
            gram(2 + p)
        else:
            shorten(0, steps, (p - 2) * pairs // 4, (p - 1) * pairs // 4)
    ones = jnp.ones((LANES, LANES), jnp.float32)

    def lane_sums(value):
        return lax.dot_general(
            ones[:SUB], value, (((1,), (1,)), ((), ())), precision=HIGHEST,
            preferred_element_type=jnp.float32,
        )[:1]

    table[pl.ds(0, 2 * count), :] = jnp.sum(gram_acc[...], axis=1)
    gram_row[...] = lane_sums(table[...])
    pl.semaphore_wait(ready.at[2], 1)
    gram_copies = spread(gram_row, gram_all, gram_send, gram_recv)
    shorten(0, steps, pairs // 2, pairs)
    shorten(1, changes, 0, pairs)
    finish(0)
    finish(1)
    first, _ = halves(table[...])
    second, third = halves(table[...] - first.astype(jnp.float32))
    late_row[...] = lax.dot_general(
        jnp.ones((SUB, 3 * LANES), jnp.bfloat16), jnp.concatenate([first, second, third], axis=1),
        (((1,), (1,)), ((), ())), preferred_element_type=jnp.float32,
    )[:1]
    late_copies = spread(late_row, late_all, late_send, late_recv)
    high, low = halves(smooth[...])
    grad[...] = jnp.dot(
        jnp.concatenate([high, low, high], axis=1), lat_mat[...],
        preferred_element_type=jnp.float32,
    )
    products = gathered(gram_row, gram_all, gram_copies)
    square = (LANES, LANES)
    on_diagonal = lax.broadcasted_iota(jnp.int32, square, 0) == lax.broadcasted_iota(jnp.int32, square, 1)
    splat[...] = jnp.dot(
        jnp.where(on_diagonal, jnp.broadcast_to(products, square), 0.0), ones,
        precision=HIGHEST, preferred_element_type=jnp.float32,
    )

    def cross(i, j):
        place = slots[i, j]
        return splat[place : place + 1, :]

    def squared(i, j):
        place = count + slots[min(i, j), max(i, j)]
        return splat[place : place + 1, :]

    def unit(place):
        return (lax.broadcasted_iota(jnp.int32, (1, LANES), 1) // SUB == place).astype(jnp.float32)

    inverse = [1.0 / cross(i, i) for i in range(pairs)]
    scaling = cross(pairs - 1, pairs - 1) / squared(pairs - 1, pairs - 1)
    alphas = [None] * pairs
    for i in reversed(range(pairs)):
        row = unit(i)
        for j in range(pairs - 1, i, -1):
            row = row - cross(i, j) * alphas[j]
        alphas[i] = inverse[i] * row
    onto = []
    for i in range(pairs):
        row = unit(pairs + i)
        for j in range(pairs):
            row = row - squared(i, j) * alphas[j]
        row = scaling * row
        for j in range(i):
            row = row + cross(j, i) * onto[j]
        onto.append(alphas[i] - inverse[i] * row)
    for i in range(pairs):
        mix[i : i + 1, :] = -onto[i]
        mix[pairs + i : pairs + i + 1, :] = scaling * alphas[i]

    for copies in (far_copies, near_copies, x_copies, halo_copies, gram_copies, late_copies):
        for copy in copies:
            copy.wait_send()
    products = gathered(late_row, late_all, late_copies)
    mixed = jnp.sum(mix[...] * products, axis=1, keepdims=True)
    factors = [
        jnp.broadcast_to(mixed[i : i + 1], (SUB, LANES)) for i in range(2 * pairs)
    ]
    ratio = jnp.broadcast_to(-scaling, (SUB, LANES))

    def combine(t, _):
        place = pl.ds(pl.multiple_of(t * SUB, SUB), SUB)
        for lane in range(lats):
            across = pl.ds(lane * LANES, LANES)
            values = [ratio * grad[place, across]]
            for i in range(pairs):
                values.append(factors[i] * steps[i, place, across])
                values.append(factors[pairs + i] * changes[i, place, across])
            while len(values) > 1:
                paired = [x + y for x, y in zip(values[::2], values[1::2])]
                values = paired + values[2 * len(paired) :]
            direc[place, across] = values[0]
        return 0

    lax.fori_loop(0, tiles, combine, 0, unroll=4)


def shards(kernels, steps, curvature):
    n_c, n_e = lax.axis_size("cuts"), lax.axis_size("event")
    _, lons, rad_len, lat_len = kernels.shape
    pairs = steps.shape[0]
    part = rad_len // n_e
    assert lons == 2 * RIM and n_e == 4 and n_c % 2 == 0
    all_rows = lons * part
    count = pairs * (pairs + 1)
    f32, bf16 = jnp.float32, jnp.bfloat16
    vmem, dma = pltpu.VMEM, pltpu.SemaphoreType.DMA
    whole = (2, RIM, part, LANES)
    per = lons // LOADS
    vmem_spec = pl.BlockSpec(memory_space=pltpu.VMEM)
    any_spec = pl.BlockSpec(memory_space=pl.ANY)
    others = n_c * n_e - 1
    assert 2 * pairs * SUB == LANES
    outs = pl.pallas_call(
        functools.partial(kernel, (n_c, n_e, pairs, rad_len, lat_len)),
        out_shape=vmem((2, all_rows, lat_len), f32),
        in_specs=[any_spec] * 3,
        out_specs=vmem_spec,
        scratch_shapes=[
            vmem((pairs, all_rows, lat_len), f32),
            vmem((pairs, all_rows, lat_len), f32),
            vmem((2, RIM, rad_len, lat_len), f32),
            vmem((2, RIM, rad_len, LANES), f32),
            vmem(whole, f32),
            vmem(whole, f32),
            vmem(whole, f32),
            vmem(whole, f32),
            vmem((per, part, LANES), f32),
            vmem(whole, f32),
            vmem(whole, f32),
            vmem((all_rows, LANES), f32),
            vmem((2 * pairs, all_rows, LANES), f32),
            vmem((rad_len, 3 * rad_len), bf16),
            vmem((2 * lat_len, 2 * LANES), bf16),
            vmem((2 * lat_len, 2 * LANES), bf16),
            vmem((3 * LANES, lat_len), bf16),
            vmem((count, SUB, LANES), f32),
            vmem((1, LANES), f32),
            vmem((others, 1, LANES), f32),
            vmem((LANES, LANES), f32),
            vmem((LANES, LANES), f32),
            vmem((2 * pairs, LANES), f32),
            vmem((1, LANES), f32),
            vmem((others, 1, LANES), f32),
            pltpu.SemaphoreType.REGULAR((3,)),
            dma((LOADS + 2,)),
            dma((2, LOADS)),
            dma((2, LOADS)),
            dma((LOADS + 1,)),
            dma((LOADS + 1,)),
            dma((LOADS,)),
            dma((2, LOADS // 2)),
            dma((others,)),
            dma((others,)),
            dma((others,)),
            dma((others,)),
        ],
        compiler_params=pltpu.CompilerParams(
            collective_id=0, has_side_effects=True, vmem_limit_bytes=61905306
        ),
    )(
        kernels.reshape(2, RIM, rad_len, lat_len),
        steps.reshape(pairs, all_rows, lat_len),
        curvature.reshape(pairs, all_rows, lat_len),
    )
    shape = (lons, part, lat_len)
    return outs[0].reshape(shape), outs[1].reshape(shape)


def solution(mesh):
    placed = (
        P("event", "cuts", None, None),
        P(None, "cuts", "event", None),
        P(None, "cuts", "event", None),
    )
    return jax.shard_map(
        shards,
        mesh=mesh,
        in_specs=placed,
        out_specs=(P("cuts", "event", None), P("cuts", "event", None)),
        check_vma=False,
    )
```

```python
import functools
import math

import jax
import jax.numpy as jnp
from jax import lax
from jax.experimental import pallas as pl
from jax.experimental.pallas import tpu as pltpu
from jax.sharding import PartitionSpec as P

RIM = 4
UNITS = 4
CHUNKS = ((0, 0, 2), (0, 2, 2), (1, 0, 2), (1, 2, 2))
LOADS = len(CHUNKS)
LANES = 128
SUB = 8
MESH = pl.DeviceIdType.MESH
HIGHEST = lax.Precision.HIGHEST


def cycle_weights():
    unscaled = [math.exp(-((column - RIM) ** 2) / 4.5) for column in range(2 * RIM + 1)]
    whole = sum(unscaled)
    return [weight / whole for weight in unscaled]


def halves(value):
    high = value.astype(jnp.bfloat16)
    return high, (value - high.astype(jnp.float32)).astype(jnp.bfloat16)


def unscaled_gauss(length, sigma):
    rows = lax.broadcasted_iota(jnp.int32, (length, length), 0)
    columns = lax.broadcasted_iota(jnp.int32, (length, length), 1)
    offset = (rows - columns).astype(jnp.float32)
    return jnp.exp(-offset * offset / (2.0 * sigma * sigma))


def factor(shape, spot_axis, length, sigma, count):
    reach = 2.25 * sigma
    pitch = (length - 1 + 2 * reach) / (count - 1)
    assert pitch < 0.54 * sigma
    spots = lax.broadcasted_iota(jnp.int32, shape, spot_axis).astype(jnp.float32)
    nodes = lax.broadcasted_iota(jnp.int32, shape, 1 - spot_axis).astype(jnp.float32)
    offset = spots - (nodes * pitch - reach)
    return jnp.exp(-offset * offset / (sigma * sigma))


def upper(pairs):
    return [(i, j) for i in range(pairs) for j in range(i, pairs)]


def kernel(
    sizes,
    kern_hbm, steps_hbm, curv_hbm, out,
    steps, changes, kern, rad, far_in, near_in, far_out, x_in, cross_in, nodes, halo_in, smooth, short,
    rad_mat, pack_mat, dual_mat, lat_mat, gram_acc, gram_row, gram_all,
    table, splat, mix, late_row, late_all,
    ready, load_sem, core_send, core_recv, x_send, x_recv, halo_send, halo_recv,
    gram_send, gram_recv, late_send, late_recv,
):
    n_c, n_e, pairs, rad_len, lat_len = sizes
    grad, direc = out.at[0], out.at[1]
    part = rad_len // n_e
    c = lax.axis_index("cuts")
    e = lax.axis_index("event")
    barrier = pltpu.get_barrier_semaphore()
    steps_left, steps_right = c >= 2, c + 2 < n_c

    def flip(place):
        return c + place * (1 - 2 * lax.rem(c // place, 2))

    def signal(semaphore, **where):
        pl.semaphore_signal(semaphore, 1, device_id=where, device_id_type=MESH)

    def enter():
        pl.semaphore_wait(barrier, n_e + steps_left.astype(jnp.int32) + steps_right.astype(jnp.int32))

        @pl.when(jnp.logical_not(steps_left) & steps_right)
        def _():
            signal(ready.at[0], cuts=c + 2)

        @pl.when(jnp.logical_not(steps_right) & steps_left)
        def _():
            signal(ready.at[1], cuts=c - 2)

    def pass_right():
        @pl.when(steps_left)
        def _():
            pl.semaphore_wait(ready.at[0], 1)

            @pl.when(steps_right)
            def _():
                signal(ready.at[0], cuts=c + 2)

    def pass_left():
        @pl.when(steps_left)
        def _():
            @pl.when(steps_right)
            def _():
                pl.semaphore_wait(ready.at[1], 1)
                signal(ready.at[1], cuts=c - 2)

            signal(ready.at[2], cuts=flip(1))

    def end_left():
        @pl.when(jnp.logical_not(steps_left))
        def _():
            @pl.when(steps_right)
            def _():
                pl.semaphore_wait(ready.at[1], 1)

            signal(ready.at[2], cuts=flip(1))

    others = []
    for mask in reversed(range(n_c)):
        where = c
        for bit in range(mask.bit_length()):
            if mask >> bit & 1:
                where = where + (flip(1 << bit) - c)
        for d in range(n_e):
            if mask or d:
                others.append({"cuts": where, "event": lax.rem(e + d, n_e)})

    sides = (lax.rem(c, 2), 1 - lax.rem(c, 2))
    chunks = [(sides[turn], pl.ds(first, size)) for turn, first, size in CHUNKS]
    loads = []
    for p, (g, ks) in enumerate(chunks):
        loads.append(pltpu.make_async_copy(kern_hbm.at[g, ks], kern.at[g, ks], load_sem.at[p]))
        loads[-1].start()
    loads.append(pltpu.make_async_copy(steps_hbm, steps, load_sem.at[LOADS]))
    loads.append(pltpu.make_async_copy(curv_hbm, changes, load_sem.at[LOADS + 1]))

    for d in range(1, n_e):
        signal(barrier, event=lax.rem(e + d, n_e))
    signal(barrier, cuts=flip(1))

    @pl.when(steps_left)
    def _():
        signal(barrier, cuts=c - 2)

    @pl.when(steps_right)
    def _():
        signal(barrier, cuts=c + 2)

    matrix = unscaled_gauss(rad_len, 3.0)
    high, low = halves(matrix / jnp.sum(matrix, axis=1, keepdims=True))
    rad_mat[...] = jnp.concatenate([high, high, low], axis=1)
    spread_out = factor((lat_len, LANES), 0, lat_len, 4.0, LANES)
    high, low = halves(spread_out)
    both = jnp.concatenate([high, low], axis=1)
    pack_mat[...] = jnp.concatenate([both, both], axis=0)
    table[...] = jnp.zeros_like(table)

    core = e + 1 - 2 * lax.rem(e, 2)
    far = lax.rem(e + 2, n_e)
    core_far = lax.rem(core + 2, n_e)

    def rows(chunk):
        return pl.ds(pl.multiple_of(chunk * part, part), part)

    def send(src, dst, send_sem, recv_sem, where):
        return pltpu.make_async_remote_copy(
            src_ref=src, dst_ref=dst, send_sem=send_sem, recv_sem=recv_sem,
            device_id=where, device_id_type=MESH,
        )

    far_copies, near_copies, x_copies, halo_copies = [], [], [], []

    def packed(value, matrix):
        high, low = halves(value)
        out = jnp.dot(
            jnp.concatenate([high, low], axis=1), matrix[...], preferred_element_type=jnp.float32
        )
        return out[:, :LANES] + out[:, LANES:]

    def exchange(p):
        g, ks = chunks[p]
        if p == 0:
            for number, (where, into) in enumerate(((far, x_in.at[g, ks]), (core_far, cross_in))):
                x_copies.append(send(
                    rad.at[g, ks, rows(where)], into, x_send.at[number], x_recv.at[number],
                    {"event": where},
                ))
                x_copies[-1].start()
        for number, (copies, chunk, into) in enumerate(
            ((far_copies, core_far, far_in), (near_copies, core, near_in))
        ):
            if p or number:
                copies.append(send(
                    rad.at[g, ks, rows(chunk)], into.at[g, ks],
                    core_send.at[number, p], core_recv.at[number, p], {"event": core},
                ))
                copies[-1].start()

    value = None
    for p in range(LOADS + 1):
        before = value
        if p < LOADS:
            g, ks = chunks[p]
            loads[p].wait()
            if p == LOADS - 1:
                for load in loads[LOADS:]:
                    load.start()
            value = packed(
                kern[g, ks].reshape(ks.size * rad_len, lat_len), pack_mat
            ).reshape(ks.size, rad_len, LANES)
        if p:
            g, ks = chunks[p - 1]
            high, low = halves(jnp.concatenate([before[k] for k in range(ks.size)], axis=1))
            done = jnp.dot(
                rad_mat[...], jnp.concatenate([high, low, high], axis=0),
                preferred_element_type=jnp.float32,
            )
            for k in range(ks.size):
                rad[g, ks.start + k] = done[:, k * LANES : (k + 1) * LANES]
            if p == 1:
                enter()
            exchange(p - 1)
    strips = part // SUB

    matrix = spread_out * jnp.sum(spread_out, axis=0, keepdims=True)
    high, low = halves(spread_out / jnp.sum(matrix, axis=1, keepdims=True))
    both = jnp.concatenate([high, low], axis=1)
    dual_mat[...] = jnp.concatenate([both, both], axis=0)
    matrix = factor((LANES, lat_len), 1, lat_len, 4.0, LANES)
    whole = jnp.sum(matrix * jnp.sum(matrix, axis=1, keepdims=True), axis=0, keepdims=True)
    high, low = halves(matrix / whole)
    lat_mat[...] = jnp.concatenate([high, high, low], axis=0)

    for copy, p in zip(far_copies, range(1, LOADS)):
        g, ks = chunks[p]
        copy.wait_recv()
        far_out[g, ks] = rad[g, ks, rows(far)] + far_in[g, ks]
        x_copies.append(send(
            far_out.at[g, ks], x_in.at[g, ks], x_send.at[p + 1], x_recv.at[p + 1],
            {"event": far},
        ))
        x_copies[-1].start()
    pass_right()

    slots = {pair: number for number, pair in enumerate(upper(pairs))}
    count = len(slots)
    groups = [(0, 1), (2, 3), tuple(range(4, pairs))]
    all_rows = steps.shape[1]
    tiles = all_rows // SUB
    lats = lat_len // LANES
    strip = tiles // UNITS

    def gram(number):
        if number == 0:
            loads[LOADS].wait()
            loads[LOADS + 1].wait()

        def scale(t, _):
            place = pl.ds(pl.multiple_of(t * SUB, SUB), SUB)
            for i in range(pairs):
                changes[i, place, :] = changes[i, place, :] * steps[i, place, :]
            return 0

        lax.fori_loop(number * strip, (number + 1) * strip, scale, 0, unroll=2)
        for group in groups:
            wanted = [(i, j) for i in group for j in range(i, pairs)]

            def body(t, sums):
                place = pl.ds(pl.multiple_of(t * SUB, SUB), SUB)
                sums = list(sums)
                for lane in range(lats):
                    across = pl.ds(lane * LANES, LANES)
                    change = {j: changes[j, place, across] for j in range(group[0], pairs)}
                    for n, i in enumerate(group):
                        step = steps[i, place, across]
                        for m, (a, b) in enumerate(wanted):
                            if a == i:
                                sums[2 * m] = sums[2 * m] + step * change[b]
                                sums[2 * m + 1] = sums[2 * m + 1] + change[i] * change[b]
                return tuple(sums)

            sums = lax.fori_loop(
                number * strip, (number + 1) * strip, body,
                tuple(jnp.zeros((SUB, LANES), jnp.float32) for _ in range(2 * len(wanted))),
            )
            for m, pair in enumerate(wanted):
                for kind in range(2):
                    place = slots[pair] + kind * count
                    if number == 0:
                        gram_acc[place] = sums[2 * m + kind]
                    else:
                        gram_acc[place] = gram_acc[place] + sums[2 * m + kind]

    def spread(row, slot_refs, sends, recvs):
        for d, other in enumerate(others):
            send(row, slot_refs.at[d], sends.at[d], recvs.at[d], other).start()
        return [
            send(row, slot_refs.at[d], sends.at[d], recvs.at[d], other)
            for d, other in enumerate(others)
        ]

    def gathered(row, slot_refs, copies):
        for copy in copies:
            copy.wait_recv()
        return row[...] + jnp.sum(slot_refs[...], axis=0)

    def arrive(p):
        g, ks = chunks[p]
        near_copies[p].wait_recv()
        base = rad[g, ks, rows(e)] + near_in[g, ks]
        if p == 0:
            x_copies[0].wait_recv()
            x_copies[1].wait_recv()
            base = base + cross_in[...]
        else:
            x_copies[p + 1].wait_recv()
        nodes[g, ks] = base + x_in[g, ks]
        halo_copies.append(send(
            nodes.at[g, ks], halo_in.at[g, ks], halo_send.at[p], halo_recv.at[p],
            {"cuts": lax.rem(c + n_c - 1 + 2 * g, n_c)},
        ))
        halo_copies[-1].start()

    def shorten(kind, vector, first, last):
        for i in range(first, last):
            short[kind * pairs + i] = packed(vector[i], dual_mat)

    weights = cycle_weights()

    def finish(turn):
        g = sides[turn]
        for p, chunk in enumerate(CHUNKS):
            if chunk[0] == turn:
                ks = chunks[p][1]
                send(
                    nodes.at[1 - g, ks], halo_in.at[1 - g, ks], halo_send.at[p], halo_recv.at[p],
                    {"event": core},
                ).wait_recv()

        def at(k):
            return k + g * (RIM - 1 - 2 * k)

        sums = [None] * (2 * pairs)
        for h in range(strips):
            place = pl.ds(h * SUB, SUB)
            padded = (
                [halo_in[1 - g, at(k), place] for k in range(RIM)]
                + [nodes[g, at(k), place] for k in range(RIM)]
                + [nodes[1 - g, at(k), place] for k in range(RIM)]
            )
            for a in range(RIM):
                value = weights[RIM] * padded[a + RIM]
                for k in range(1, RIM + 1):
                    value = value + weights[RIM + k] * (padded[a + RIM - k] + padded[a + RIM + k])
                spot = pl.ds(pl.multiple_of((g * RIM + at(a)) * part + h * SUB, SUB), SUB)
                smooth[spot, :] = value
                for n in range(2 * pairs):
                    term = value * short[n, spot, :]
                    sums[n] = term if sums[n] is None else sums[n] + term
        for n in range(2 * pairs):
            place = pl.ds(n * SUB, SUB)
            table[place, :] = sums[n] if turn == 0 else table[place, :] + sums[n]

    pass_left()
    end_left()
    begun = 0
    for p in range(LOADS):
        arrive(p)
        if p < UNITS // 2:
            gram(p)
        else:
            shorten(0, steps, begun, begun + 2)
            begun += 2
    for number in range(UNITS // 2, UNITS):
        gram(number)
    ones = jnp.ones((LANES, LANES), jnp.float32)

    def lane_sums(value):
        return lax.dot_general(
            ones[:SUB], value, (((1,), (1,)), ((), ())), precision=HIGHEST,
            preferred_element_type=jnp.float32,
        )[:1]

    table[pl.ds(0, 2 * count), :] = jnp.sum(gram_acc[...], axis=1)
    gram_row[...] = lane_sums(table[...])
    pl.semaphore_wait(ready.at[2], 1)
    gram_copies = spread(gram_row, gram_all, gram_send, gram_recv)
    shorten(0, steps, begun, pairs)
    shorten(1, changes, 0, pairs)
    finish(0)
    finish(1)
    first, _ = halves(table[...])
    second, third = halves(table[...] - first.astype(jnp.float32))
    late_row[...] = lax.dot_general(
        jnp.ones((SUB, 3 * LANES), jnp.bfloat16), jnp.concatenate([first, second, third], axis=1),
        (((1,), (1,)), ((), ())), preferred_element_type=jnp.float32,
    )[:1]
    late_copies = spread(late_row, late_all, late_send, late_recv)
    high, low = halves(smooth[...])
    grad[...] = jnp.dot(
        jnp.concatenate([high, low, high], axis=1), lat_mat[...],
        preferred_element_type=jnp.float32,
    )
    products = gathered(gram_row, gram_all, gram_copies)
    square = (LANES, LANES)
    on_diagonal = lax.broadcasted_iota(jnp.int32, square, 0) == lax.broadcasted_iota(jnp.int32, square, 1)
    splat[...] = jnp.dot(
        jnp.where(on_diagonal, jnp.broadcast_to(products, square), 0.0), ones,
        precision=HIGHEST, preferred_element_type=jnp.float32,
    )

    def cross(i, j):
        place = slots[i, j]
        return splat[place : place + 1, :]

    def squared(i, j):
        place = count + slots[min(i, j), max(i, j)]
        return splat[place : place + 1, :]

    def unit(place):
        return (lax.broadcasted_iota(jnp.int32, (1, LANES), 1) // SUB == place).astype(jnp.float32)

    inverse = [1.0 / cross(i, i) for i in range(pairs)]
    scaling = cross(pairs - 1, pairs - 1) / squared(pairs - 1, pairs - 1)
    alphas = [None] * pairs
    for i in reversed(range(pairs)):
        row = unit(i)
        for j in range(pairs - 1, i, -1):
            row = row - cross(i, j) * alphas[j]
        alphas[i] = inverse[i] * row
    onto = []
    for i in range(pairs):
        row = unit(pairs + i)
        for j in range(pairs):
            row = row - squared(i, j) * alphas[j]
        row = scaling * row
        for j in range(i):
            row = row + cross(j, i) * onto[j]
        onto.append(alphas[i] - inverse[i] * row)
    for i in range(pairs):
        mix[i : i + 1, :] = -onto[i]
        mix[pairs + i : pairs + i + 1, :] = scaling * alphas[i]

    for copies in (far_copies, near_copies, x_copies, halo_copies, gram_copies, late_copies):
        for copy in copies:
            copy.wait_send()
    products = gathered(late_row, late_all, late_copies)
    mixed = jnp.sum(mix[...] * products, axis=1, keepdims=True)
    factors = [
        jnp.broadcast_to(mixed[i : i + 1], (SUB, LANES)) for i in range(2 * pairs)
    ]
    ratio = jnp.broadcast_to(-scaling, (SUB, LANES))

    def combine(t, _):
        place = pl.ds(pl.multiple_of(t * SUB, SUB), SUB)
        for lane in range(lats):
            across = pl.ds(lane * LANES, LANES)
            values = [ratio * grad[place, across]]
            for i in range(pairs):
                values.append(factors[i] * steps[i, place, across])
                values.append(factors[pairs + i] * changes[i, place, across])
            while len(values) > 1:
                paired = [x + y for x, y in zip(values[::2], values[1::2])]
                values = paired + values[2 * len(paired) :]
            direc[place, across] = values[0]
        return 0

    lax.fori_loop(0, tiles, combine, 0, unroll=8)


def shards(kernels, steps, curvature):
    n_c, n_e = lax.axis_size("cuts"), lax.axis_size("event")
    _, lons, rad_len, lat_len = kernels.shape
    pairs = steps.shape[0]
    part = rad_len // n_e
    assert lons == 2 * RIM and n_e == 4 and n_c % 2 == 0
    all_rows = lons * part
    count = pairs * (pairs + 1)
    f32, bf16 = jnp.float32, jnp.bfloat16
    vmem, dma = pltpu.VMEM, pltpu.SemaphoreType.DMA
    whole = (2, RIM, part, LANES)
    vmem_spec = pl.BlockSpec(memory_space=pltpu.VMEM)
    any_spec = pl.BlockSpec(memory_space=pl.ANY)
    others = n_c * n_e - 1
    assert 2 * pairs * SUB == LANES
    outs = pl.pallas_call(
        functools.partial(kernel, (n_c, n_e, pairs, rad_len, lat_len)),
        out_shape=vmem((2, all_rows, lat_len), f32),
        in_specs=[any_spec] * 3,
        out_specs=vmem_spec,
        scratch_shapes=[
            vmem((pairs, all_rows, lat_len), f32),
            vmem((pairs, all_rows, lat_len), f32),
            vmem((2, RIM, rad_len, lat_len), f32),
            vmem((2, RIM, rad_len, LANES), f32),
            vmem(whole, f32),
            vmem(whole, f32),
            vmem(whole, f32),
            vmem(whole, f32),
            vmem((CHUNKS[0][2], part, LANES), f32),
            vmem(whole, f32),
            vmem(whole, f32),
            vmem((all_rows, LANES), f32),
            vmem((2 * pairs, all_rows, LANES), f32),
            vmem((rad_len, 3 * rad_len), bf16),
            vmem((2 * lat_len, 2 * LANES), bf16),
            vmem((2 * lat_len, 2 * LANES), bf16),
            vmem((3 * LANES, lat_len), bf16),
            vmem((count, SUB, LANES), f32),
            vmem((1, LANES), f32),
            vmem((others, 1, LANES), f32),
            vmem((LANES, LANES), f32),
            vmem((LANES, LANES), f32),
            vmem((2 * pairs, LANES), f32),
            vmem((1, LANES), f32),
            vmem((others, 1, LANES), f32),
            pltpu.SemaphoreType.REGULAR((3,)),
            dma((LOADS + 2,)),
            dma((2, LOADS)),
            dma((2, LOADS)),
            dma((LOADS + 1,)),
            dma((LOADS + 1,)),
            dma((LOADS,)),
            dma((LOADS,)),
            dma((others,)),
            dma((others,)),
            dma((others,)),
            dma((others,)),
        ],
        compiler_params=pltpu.CompilerParams(
            collective_id=0, has_side_effects=True, vmem_limit_bytes=61905306
        ),
    )(
        kernels.reshape(2, RIM, rad_len, lat_len),
        steps.reshape(pairs, all_rows, lat_len),
        curvature.reshape(pairs, all_rows, lat_len),
    )
    shape = (lons, part, lat_len)
    return outs[0].reshape(shape), outs[1].reshape(shape)


def solution(mesh):
    placed = (
        P("event", "cuts", None, None),
        P(None, "cuts", "event", None),
        P(None, "cuts", "event", None),
    )
    return jax.shard_map(
        shards,
        mesh=mesh,
        in_specs=placed,
        out_specs=(P("cuts", "event", None), P("cuts", "event", None)),
        check_vma=False,
    )
```

```python
import functools
import math

import jax
import jax.numpy as jnp
from jax import lax
from jax.experimental import pallas as pl
from jax.experimental.pallas import tpu as pltpu
from jax.sharding import PartitionSpec as P

RIM = 4
UNITS = 4
CHUNKS = ((0, 0, 2), (0, 2, 2), (1, 0, 2), (1, 2, 2))
LOADS = len(CHUNKS)
LANES = 128
SUB = 8
MESH = pl.DeviceIdType.MESH
HIGHEST = lax.Precision.HIGHEST


def cycle_weights():
    unscaled = [math.exp(-((column - RIM) ** 2) / 4.5) for column in range(2 * RIM + 1)]
    whole = sum(unscaled)
    return [weight / whole for weight in unscaled]


def halves(value):
    high = value.astype(jnp.bfloat16)
    return high, (value - high.astype(jnp.float32)).astype(jnp.bfloat16)


def unscaled_gauss(length, sigma):
    rows = lax.broadcasted_iota(jnp.int32, (length, length), 0)
    columns = lax.broadcasted_iota(jnp.int32, (length, length), 1)
    offset = (rows - columns).astype(jnp.float32)
    return jnp.exp(-offset * offset / (2.0 * sigma * sigma))


def factor(shape, spot_axis, length, sigma, count):
    reach = 2.25 * sigma
    pitch = (length - 1 + 2 * reach) / (count - 1)
    assert pitch < 0.54 * sigma
    spots = lax.broadcasted_iota(jnp.int32, shape, spot_axis).astype(jnp.float32)
    nodes = lax.broadcasted_iota(jnp.int32, shape, 1 - spot_axis).astype(jnp.float32)
    offset = spots - (nodes * pitch - reach)
    return jnp.exp(-offset * offset / (sigma * sigma))


def upper(pairs):
    return [(i, j) for i in range(pairs) for j in range(i, pairs)]


def kernel(
    sizes,
    kern_hbm, steps_hbm, curv_hbm, out,
    steps, changes, kern, rad, far_in, near_in, far_out, x_in, cross_in, nodes, halo_in, smooth, short,
    rad_mat, pack_mat, dual_mat, lat_mat, gram_acc, gram_row, gram_all,
    table, splat, mix, late_row, late_all,
    ready, load_sem, core_send, core_recv, x_send, x_recv, halo_send, halo_recv,
    gram_send, gram_recv, late_send, late_recv,
):
    n_c, n_e, pairs, rad_len, lat_len = sizes
    grad, direc = out.at[0], out.at[1]
    part = rad_len // n_e
    c = lax.axis_index("cuts")
    e = lax.axis_index("event")
    barrier = pltpu.get_barrier_semaphore()
    steps_left, steps_right = c >= 2, c + 2 < n_c

    def flip(place):
        return c + place * (1 - 2 * lax.rem(c // place, 2))

    def signal(semaphore, **where):
        pl.semaphore_signal(semaphore, 1, device_id=where, device_id_type=MESH)

    def enter():
        pl.semaphore_wait(barrier, n_e + steps_left.astype(jnp.int32) + steps_right.astype(jnp.int32))

        @pl.when(jnp.logical_not(steps_left) & steps_right)
        def _():
            signal(ready.at[0], cuts=c + 2)

        @pl.when(jnp.logical_not(steps_right) & steps_left)
        def _():
            signal(ready.at[1], cuts=c - 2)

    def pass_right():
        @pl.when(steps_left)
        def _():
            pl.semaphore_wait(ready.at[0], 1)

            @pl.when(steps_right)
            def _():
                signal(ready.at[0], cuts=c + 2)

    def pass_left():
        @pl.when(steps_left)
        def _():
            @pl.when(steps_right)
            def _():
                pl.semaphore_wait(ready.at[1], 1)
                signal(ready.at[1], cuts=c - 2)

            signal(ready.at[2], cuts=flip(1))

    def end_left():
        @pl.when(jnp.logical_not(steps_left))
        def _():
            @pl.when(steps_right)
            def _():
                pl.semaphore_wait(ready.at[1], 1)

            signal(ready.at[2], cuts=flip(1))

    others = []
    for mask in reversed(range(n_c)):
        where = c
        for bit in range(mask.bit_length()):
            if mask >> bit & 1:
                where = where + (flip(1 << bit) - c)
        for d in range(n_e):
            if mask or d:
                others.append({"cuts": where, "event": lax.rem(e + d, n_e)})

    sides = (lax.rem(c, 2), 1 - lax.rem(c, 2))
    chunks = [(sides[turn], pl.ds(first, size)) for turn, first, size in CHUNKS]
    loads = []
    for p, (g, ks) in enumerate(chunks):
        loads.append(pltpu.make_async_copy(kern_hbm.at[g, ks], kern.at[g, ks], load_sem.at[p]))
        loads[-1].start()
    loads.append(pltpu.make_async_copy(steps_hbm, steps, load_sem.at[LOADS]))
    loads.append(pltpu.make_async_copy(curv_hbm, changes, load_sem.at[LOADS + 1]))

    for d in range(1, n_e):
        signal(barrier, event=lax.rem(e + d, n_e))
    signal(barrier, cuts=flip(1))

    @pl.when(steps_left)
    def _():
        signal(barrier, cuts=c - 2)

    @pl.when(steps_right)
    def _():
        signal(barrier, cuts=c + 2)

    matrix = unscaled_gauss(rad_len, 3.0)
    high, low = halves(matrix / jnp.sum(matrix, axis=1, keepdims=True))
    rad_mat[...] = jnp.concatenate([high, high, low], axis=1)
    spread_out = factor((lat_len, LANES), 0, lat_len, 4.0, LANES)
    high, low = halves(spread_out)
    both = jnp.concatenate([high, low], axis=1)
    pack_mat[...] = jnp.concatenate([both, both], axis=0)
    table[...] = jnp.zeros_like(table)

    core = e + 1 - 2 * lax.rem(e, 2)
    far = lax.rem(e + 2, n_e)
    core_far = lax.rem(core + 2, n_e)

    def rows(chunk):
        return pl.ds(pl.multiple_of(chunk * part, part), part)

    def send(src, dst, send_sem, recv_sem, where):
        return pltpu.make_async_remote_copy(
            src_ref=src, dst_ref=dst, send_sem=send_sem, recv_sem=recv_sem,
            device_id=where, device_id_type=MESH,
        )

    far_copies, near_copies, x_copies, halo_copies = [], [], [], []

    def packed(value, matrix):
        high, low = halves(value)
        out = jnp.dot(
            jnp.concatenate([high, low], axis=1), matrix[...], preferred_element_type=jnp.float32
        )
        return out[:, :LANES] + out[:, LANES:]

    def exchange(p):
        g, ks = chunks[p]
        if p == 0:
            for number, (where, into) in enumerate(((far, x_in.at[g, ks]), (core_far, cross_in))):
                x_copies.append(send(
                    rad.at[g, ks, rows(where)], into, x_send.at[number], x_recv.at[number],
                    {"event": where},
                ))
                x_copies[-1].start()
        for number, (copies, chunk, into) in enumerate(
            ((far_copies, core_far, far_in), (near_copies, core, near_in))
        ):
            if p or number:
                copies.append(send(
                    rad.at[g, ks, rows(chunk)], into.at[g, ks],
                    core_send.at[number, p], core_recv.at[number, p], {"event": core},
                ))
                copies[-1].start()

    value = None
    for p in range(LOADS + 1):
        before = value
        if p < LOADS:
            g, ks = chunks[p]
            loads[p].wait()
            if p == LOADS - 1:
                for load in loads[LOADS:]:
                    load.start()
            value = packed(
                kern[g, ks].reshape(ks.size * rad_len, lat_len), pack_mat
            ).reshape(ks.size, rad_len, LANES)
        if p:
            g, ks = chunks[p - 1]
            high, low = halves(jnp.concatenate([before[k] for k in range(ks.size)], axis=1))
            done = jnp.dot(
                rad_mat[...], jnp.concatenate([high, low, high], axis=0),
                preferred_element_type=jnp.float32,
            )
            for k in range(ks.size):
                rad[g, ks.start + k] = done[:, k * LANES : (k + 1) * LANES]
            if p == 1:
                enter()
            exchange(p - 1)
    strips = part // SUB

    matrix = spread_out * jnp.sum(spread_out, axis=0, keepdims=True)
    high, low = halves(spread_out / jnp.sum(matrix, axis=1, keepdims=True))
    both = jnp.concatenate([high, low], axis=1)
    dual_mat[...] = jnp.concatenate([both, both], axis=0)
    matrix = factor((LANES, lat_len), 1, lat_len, 4.0, LANES)
    whole = jnp.sum(matrix * jnp.sum(matrix, axis=1, keepdims=True), axis=0, keepdims=True)
    high, low = halves(matrix / whole)
    lat_mat[...] = jnp.concatenate([high, high, low], axis=0)

    for copy, p in zip(far_copies, range(1, LOADS)):
        g, ks = chunks[p]
        copy.wait_recv()
        far_out[g, ks] = rad[g, ks, rows(far)] + far_in[g, ks]
        x_copies.append(send(
            far_out.at[g, ks], x_in.at[g, ks], x_send.at[p + 1], x_recv.at[p + 1],
            {"event": far},
        ))
        x_copies[-1].start()
    pass_right()

    slots = {pair: number for number, pair in enumerate(upper(pairs))}
    count = len(slots)
    groups = [(0, 1), (2, 3), tuple(range(4, pairs))]
    all_rows = steps.shape[1]
    tiles = all_rows // SUB
    lats = lat_len // LANES
    strip = tiles // UNITS

    def gram(number):
        if number == 0:
            loads[LOADS].wait()
            loads[LOADS + 1].wait()

        def scale(t, _):
            place = pl.ds(pl.multiple_of(t * SUB, SUB), SUB)
            for i in range(pairs):
                changes[i, place, :] = changes[i, place, :] * steps[i, place, :]
            return 0

        lax.fori_loop(number * strip, (number + 1) * strip, scale, 0, unroll=2)
        for group in groups:
            wanted = [(i, j) for i in group for j in range(i, pairs)]

            def body(t, sums):
                place = pl.ds(pl.multiple_of(t * SUB, SUB), SUB)
                sums = list(sums)
                for lane in range(lats):
                    across = pl.ds(lane * LANES, LANES)
                    change = {j: changes[j, place, across] for j in range(group[0], pairs)}
                    for n, i in enumerate(group):
                        step = steps[i, place, across]
                        for m, (a, b) in enumerate(wanted):
                            if a == i:
                                sums[2 * m] = sums[2 * m] + step * change[b]
                                sums[2 * m + 1] = sums[2 * m + 1] + change[i] * change[b]
                return tuple(sums)

            sums = lax.fori_loop(
                number * strip, (number + 1) * strip, body,
                tuple(jnp.zeros((SUB, LANES), jnp.float32) for _ in range(2 * len(wanted))),
            )
            for m, pair in enumerate(wanted):
                for kind in range(2):
                    place = slots[pair] + kind * count
                    if number == 0:
                        gram_acc[place] = sums[2 * m + kind]
                    else:
                        gram_acc[place] = gram_acc[place] + sums[2 * m + kind]

    def spread(row, slot_refs, sent, landed):
        for d, other in enumerate(others):
            send(row, slot_refs.at[d], sent, landed, other).start()
        return send(slot_refs, slot_refs, sent, landed, others[0])

    def gathered(row, slot_refs, copy):
        copy.wait_recv()
        return row[...] + jnp.sum(slot_refs[...], axis=0)

    def arrive(p):
        g, ks = chunks[p]
        near_copies[p].wait_recv()
        base = rad[g, ks, rows(e)] + near_in[g, ks]
        if p == 0:
            x_copies[0].wait_recv()
            x_copies[1].wait_recv()
            base = base + cross_in[...]
        else:
            x_copies[p + 1].wait_recv()
        nodes[g, ks] = base + x_in[g, ks]
        halo_copies.append(send(
            nodes.at[g, ks], halo_in.at[g, ks], halo_send.at[p], halo_recv.at[p],
            {"cuts": lax.rem(c + n_c - 1 + 2 * g, n_c)},
        ))
        halo_copies[-1].start()

    def shorten(kind, vector, first, last):
        for i in range(first, last):
            short[kind * pairs + i] = packed(vector[i], dual_mat)

    weights = cycle_weights()

    def finish(turn):
        g = sides[turn]
        for p, chunk in enumerate(CHUNKS):
            if chunk[0] == turn:
                ks = chunks[p][1]
                send(
                    nodes.at[1 - g, ks], halo_in.at[1 - g, ks], halo_send.at[p], halo_recv.at[p],
                    {"event": core},
                ).wait_recv()

        def at(k):
            return k + g * (RIM - 1 - 2 * k)

        sums = [None] * (2 * pairs)
        for h in range(strips):
            place = pl.ds(h * SUB, SUB)
            padded = (
                [halo_in[1 - g, at(k), place] for k in range(RIM)]
                + [nodes[g, at(k), place] for k in range(RIM)]
                + [nodes[1 - g, at(k), place] for k in range(RIM)]
            )
            for a in range(RIM):
                value = weights[RIM] * padded[a + RIM]
                for k in range(1, RIM + 1):
                    value = value + weights[RIM + k] * (padded[a + RIM - k] + padded[a + RIM + k])
                spot = pl.ds(pl.multiple_of((g * RIM + at(a)) * part + h * SUB, SUB), SUB)
                smooth[spot, :] = value
                for n in range(2 * pairs):
                    term = value * short[n, spot, :]
                    sums[n] = term if sums[n] is None else sums[n] + term
        for n in range(2 * pairs):
            place = pl.ds(n * SUB, SUB)
            table[place, :] = sums[n] if turn == 0 else table[place, :] + sums[n]

    pass_left()
    end_left()
    begun = 0
    for p in range(LOADS):
        arrive(p)
        if p < UNITS // 2:
            gram(p)
        else:
            shorten(0, steps, begun, begun + 2)
            begun += 2
    for number in range(UNITS // 2, UNITS):
        gram(number)
    ones = jnp.ones((LANES, LANES), jnp.float32)

    def lane_sums(value):
        return lax.dot_general(
            ones[:SUB], value, (((1,), (1,)), ((), ())), precision=HIGHEST,
            preferred_element_type=jnp.float32,
        )[:1]

    table[pl.ds(0, 2 * count), :] = jnp.sum(gram_acc[...], axis=1)
    gram_row[...] = lane_sums(table[...])
    pl.semaphore_wait(ready.at[2], 1)
    gram_copies = spread(gram_row, gram_all, gram_send.at[0], gram_recv.at[0])
    shorten(0, steps, begun, pairs)
    shorten(1, changes, 0, pairs)
    finish(0)
    finish(1)
    first, _ = halves(table[...])
    second, third = halves(table[...] - first.astype(jnp.float32))
    late_row[...] = lax.dot_general(
        jnp.ones((SUB, 3 * LANES), jnp.bfloat16), jnp.concatenate([first, second, third], axis=1),
        (((1,), (1,)), ((), ())), preferred_element_type=jnp.float32,
    )[:1]
    late_copies = spread(late_row, late_all, late_send.at[0], late_recv.at[0])
    high, low = halves(smooth[...])
    grad[...] = jnp.dot(
        jnp.concatenate([high, low, high], axis=1), lat_mat[...],
        preferred_element_type=jnp.float32,
    )
    products = gathered(gram_row, gram_all, gram_copies)
    square = (LANES, LANES)
    on_diagonal = lax.broadcasted_iota(jnp.int32, square, 0) == lax.broadcasted_iota(jnp.int32, square, 1)
    splat[...] = jnp.dot(
        jnp.where(on_diagonal, jnp.broadcast_to(products, square), 0.0), ones,
        precision=HIGHEST, preferred_element_type=jnp.float32,
    )

    def cross(i, j):
        place = slots[i, j]
        return splat[place : place + 1, :]

    def squared(i, j):
        place = count + slots[min(i, j), max(i, j)]
        return splat[place : place + 1, :]

    def unit(place):
        return (lax.broadcasted_iota(jnp.int32, (1, LANES), 1) // SUB == place).astype(jnp.float32)

    inverse = [1.0 / cross(i, i) for i in range(pairs)]
    scaling = cross(pairs - 1, pairs - 1) / squared(pairs - 1, pairs - 1)
    alphas = [None] * pairs
    for i in reversed(range(pairs)):
        row = unit(i)
        for j in range(pairs - 1, i, -1):
            row = row - cross(i, j) * alphas[j]
        alphas[i] = inverse[i] * row
    onto = []
    for i in range(pairs):
        row = unit(pairs + i)
        for j in range(pairs):
            row = row - squared(i, j) * alphas[j]
        row = scaling * row
        for j in range(i):
            row = row + cross(j, i) * onto[j]
        onto.append(alphas[i] - inverse[i] * row)
    for i in range(pairs):
        mix[i : i + 1, :] = -onto[i]
        mix[pairs + i : pairs + i + 1, :] = scaling * alphas[i]

    for copies in (far_copies, near_copies, x_copies, halo_copies, (gram_copies, late_copies)):
        for copy in copies:
            copy.wait_send()
    products = gathered(late_row, late_all, late_copies)
    mixed = jnp.sum(mix[...] * products, axis=1, keepdims=True)
    factors = [
        jnp.broadcast_to(mixed[i : i + 1], (SUB, LANES)) for i in range(2 * pairs)
    ]
    ratio = jnp.broadcast_to(-scaling, (SUB, LANES))

    def combine(t, _):
        place = pl.ds(pl.multiple_of(t * SUB, SUB), SUB)
        for lane in range(lats):
            across = pl.ds(lane * LANES, LANES)
            values = [ratio * grad[place, across]]
            for i in range(pairs):
                values.append(factors[i] * steps[i, place, across])
                values.append(factors[pairs + i] * changes[i, place, across])
            while len(values) > 1:
                paired = [x + y for x, y in zip(values[::2], values[1::2])]
                values = paired + values[2 * len(paired) :]
            direc[place, across] = values[0]
        return 0

    lax.fori_loop(0, tiles, combine, 0, unroll=8)


def shards(kernels, steps, curvature):
    n_c, n_e = lax.axis_size("cuts"), lax.axis_size("event")
    _, lons, rad_len, lat_len = kernels.shape
    pairs = steps.shape[0]
    part = rad_len // n_e
    assert lons == 2 * RIM and n_e == 4 and n_c % 2 == 0
    all_rows = lons * part
    count = pairs * (pairs + 1)
    f32, bf16 = jnp.float32, jnp.bfloat16
    vmem, dma = pltpu.VMEM, pltpu.SemaphoreType.DMA
    whole = (2, RIM, part, LANES)
    vmem_spec = pl.BlockSpec(memory_space=pltpu.VMEM)
    any_spec = pl.BlockSpec(memory_space=pl.ANY)
    others = n_c * n_e - 1
    assert 2 * pairs * SUB == LANES
    outs = pl.pallas_call(
        functools.partial(kernel, (n_c, n_e, pairs, rad_len, lat_len)),
        out_shape=vmem((2, all_rows, lat_len), f32),
        in_specs=[any_spec] * 3,
        out_specs=vmem_spec,
        scratch_shapes=[
            vmem((pairs, all_rows, lat_len), f32),
            vmem((pairs, all_rows, lat_len), f32),
            vmem((2, RIM, rad_len, lat_len), f32),
            vmem((2, RIM, rad_len, LANES), f32),
            vmem(whole, f32),
            vmem(whole, f32),
            vmem(whole, f32),
            vmem(whole, f32),
            vmem((CHUNKS[0][2], part, LANES), f32),
            vmem(whole, f32),
            vmem(whole, f32),
            vmem((all_rows, LANES), f32),
            vmem((2 * pairs, all_rows, LANES), f32),
            vmem((rad_len, 3 * rad_len), bf16),
            vmem((2 * lat_len, 2 * LANES), bf16),
            vmem((2 * lat_len, 2 * LANES), bf16),
            vmem((3 * LANES, lat_len), bf16),
            vmem((count, SUB, LANES), f32),
            vmem((1, LANES), f32),
            vmem((others, 1, LANES), f32),
            vmem((LANES, LANES), f32),
            vmem((LANES, LANES), f32),
            vmem((2 * pairs, LANES), f32),
            vmem((1, LANES), f32),
            vmem((others, 1, LANES), f32),
            pltpu.SemaphoreType.REGULAR((3,)),
            dma((LOADS + 2,)),
            dma((2, LOADS)),
            dma((2, LOADS)),
            dma((LOADS + 1,)),
            dma((LOADS + 1,)),
            dma((LOADS,)),
            dma((LOADS,)),
            dma((1,)),
            dma((1,)),
            dma((1,)),
            dma((1,)),
        ],
        compiler_params=pltpu.CompilerParams(
            collective_id=0, has_side_effects=True, vmem_limit_bytes=61905306
        ),
    )(
        kernels.reshape(2, RIM, rad_len, lat_len),
        steps.reshape(pairs, all_rows, lat_len),
        curvature.reshape(pairs, all_rows, lat_len),
    )
    shape = (lons, part, lat_len)
    return outs[0].reshape(shape), outs[1].reshape(shape)


def solution(mesh):
    placed = (
        P("event", "cuts", None, None),
        P(None, "cuts", "event", None),
        P(None, "cuts", "event", None),
    )
    return jax.shard_map(
        shards,
        mesh=mesh,
        in_specs=placed,
        out_specs=(P("cuts", "event", None), P("cuts", "event", None)),
        check_vma=False,
    )
```

```python
import functools
import math

import jax
import jax.numpy as jnp
from jax import lax
from jax.experimental import pallas as pl
from jax.experimental.pallas import tpu as pltpu
from jax.sharding import PartitionSpec as P

RIM = 4
UNITS = 4
CHUNKS = ((0, 0, 2), (0, 2, 2), (1, 0, 2), (1, 2, 2))
LOADS = len(CHUNKS)
LANES = 128
SUB = 8
MESH = pl.DeviceIdType.MESH
HIGHEST = lax.Precision.HIGHEST


def cycle_weights():
    unscaled = [math.exp(-((column - RIM) ** 2) / 4.5) for column in range(2 * RIM + 1)]
    whole = sum(unscaled)
    return [weight / whole for weight in unscaled]


def halves(value):
    high = value.astype(jnp.bfloat16)
    return high, (value - high.astype(jnp.float32)).astype(jnp.bfloat16)


def unscaled_gauss(length, sigma):
    rows = lax.broadcasted_iota(jnp.int32, (length, length), 0)
    columns = lax.broadcasted_iota(jnp.int32, (length, length), 1)
    offset = (rows - columns).astype(jnp.float32)
    return jnp.exp(-offset * offset / (2.0 * sigma * sigma))


def factor(shape, spot_axis, length, sigma, count):
    reach = 2.25 * sigma
    pitch = (length - 1 + 2 * reach) / (count - 1)
    assert pitch < 0.54 * sigma
    spots = lax.broadcasted_iota(jnp.int32, shape, spot_axis).astype(jnp.float32)
    nodes = lax.broadcasted_iota(jnp.int32, shape, 1 - spot_axis).astype(jnp.float32)
    offset = spots - (nodes * pitch - reach)
    return jnp.exp(-offset * offset / (sigma * sigma))


def upper(pairs):
    return [(i, j) for i in range(pairs) for j in range(i, pairs)]


def kernel(
    sizes,
    kern_hbm, steps_hbm, curv_hbm, out,
    steps, changes, kern, rad, far_in, near_in, far_out, x_in, cross_in, nodes, halo_in, smooth, short,
    rad_mat, pack_mat, dual_mat, lat_mat, gram_acc, gram_row, gram_all,
    table, splat, mix, late_row, late_all,
    ready, load_sem, core_send, core_recv, x_send, x_recv, halo_send, halo_recv,
    gram_send, gram_recv, late_send, late_recv,
):
    n_c, n_e, pairs, rad_len, lat_len = sizes
    grad, direc = out.at[0], out.at[1]
    part = rad_len // n_e
    c = lax.axis_index("cuts")
    e = lax.axis_index("event")
    barrier = pltpu.get_barrier_semaphore()
    steps_left, steps_right = c >= 2, c + 2 < n_c

    def flip(place):
        return c + place * (1 - 2 * lax.rem(c // place, 2))

    def signal(semaphore, **where):
        pl.semaphore_signal(semaphore, 1, device_id=where, device_id_type=MESH)

    def enter():
        pl.semaphore_wait(barrier, n_e + steps_left.astype(jnp.int32) + steps_right.astype(jnp.int32))

        @pl.when(jnp.logical_not(steps_left) & steps_right)
        def _():
            signal(ready.at[0], cuts=c + 2)

        @pl.when(jnp.logical_not(steps_right) & steps_left)
        def _():
            signal(ready.at[1], cuts=c - 2)

    def pass_right():
        @pl.when(steps_left)
        def _():
            pl.semaphore_wait(ready.at[0], 1)

            @pl.when(steps_right)
            def _():
                signal(ready.at[0], cuts=c + 2)

    def pass_left():
        @pl.when(steps_left)
        def _():
            @pl.when(steps_right)
            def _():
                pl.semaphore_wait(ready.at[1], 1)
                signal(ready.at[1], cuts=c - 2)

            signal(ready.at[2], cuts=flip(1))

    def end_left():
        @pl.when(jnp.logical_not(steps_left))
        def _():
            @pl.when(steps_right)
            def _():
                pl.semaphore_wait(ready.at[1], 1)

            signal(ready.at[2], cuts=flip(1))

    others = []
    for mask in reversed(range(n_c)):
        where = c
        for bit in range(mask.bit_length()):
            if mask >> bit & 1:
                where = where + (flip(1 << bit) - c)
        for d in range(n_e):
            if mask or d:
                others.append({"cuts": where, "event": lax.rem(e + d, n_e)})

    sides = (lax.rem(c, 2), 1 - lax.rem(c, 2))
    chunks = [(sides[turn], pl.ds(first, size)) for turn, first, size in CHUNKS]
    loads = []
    for p, (g, ks) in enumerate(chunks):
        loads.append(pltpu.make_async_copy(kern_hbm.at[g, ks], kern.at[g, ks], load_sem.at[p]))
        loads[-1].start()
    loads.append(pltpu.make_async_copy(steps_hbm, steps, load_sem.at[LOADS]))
    loads.append(pltpu.make_async_copy(curv_hbm, changes, load_sem.at[LOADS + 1]))

    for d in range(1, n_e):
        signal(barrier, event=lax.rem(e + d, n_e))
    signal(barrier, cuts=flip(1))

    @pl.when(steps_left)
    def _():
        signal(barrier, cuts=c - 2)

    @pl.when(steps_right)
    def _():
        signal(barrier, cuts=c + 2)

    matrix = unscaled_gauss(rad_len, 3.0)
    high, low = halves(matrix / jnp.sum(matrix, axis=1, keepdims=True))
    rad_mat[...] = jnp.concatenate([high, high, low], axis=1)
    spread_out = factor((lat_len, LANES), 0, lat_len, 4.0, LANES)
    high, low = halves(spread_out)
    both = jnp.concatenate([high, low], axis=1)
    pack_mat[...] = jnp.concatenate([both, both], axis=0)
    table[...] = jnp.zeros_like(table)

    core = e + 1 - 2 * lax.rem(e, 2)
    far = lax.rem(e + 2, n_e)
    core_far = lax.rem(core + 2, n_e)

    def rows(chunk):
        return pl.ds(pl.multiple_of(chunk * part, part), part)

    def send(src, dst, send_sem, recv_sem, where):
        return pltpu.make_async_remote_copy(
            src_ref=src, dst_ref=dst, send_sem=send_sem, recv_sem=recv_sem,
            device_id=where, device_id_type=MESH,
        )

    far_copies, near_copies, x_copies, halo_copies = [], [], [], []

    def packed(value, matrix):
        high, low = halves(value)
        out = jnp.dot(
            jnp.concatenate([high, low], axis=1), matrix[...], preferred_element_type=jnp.float32
        )
        return out[:, :LANES] + out[:, LANES:]

    def exchange(p):
        g, ks = chunks[p]
        if p == 0:
            for number, (where, into) in enumerate(((far, x_in.at[g, ks]), (core_far, cross_in))):
                x_copies.append(send(
                    rad.at[g, ks, rows(where)], into, x_send.at[number], x_recv.at[number],
                    {"event": where},
                ))
                x_copies[-1].start()
        for number, (copies, chunk, into) in enumerate(
            ((far_copies, core_far, far_in), (near_copies, core, near_in))
        ):
            if p or number:
                copies.append(send(
                    rad.at[g, ks, rows(chunk)], into.at[g, ks],
                    core_send.at[0 if number else p], core_recv.at[0 if number else p], {"event": core},
                ))
                copies[-1].start()

    value = None
    for p in range(LOADS + 1):
        before = value
        if p < LOADS:
            g, ks = chunks[p]
            loads[p].wait()
            if p == LOADS - 1:
                for load in loads[LOADS:]:
                    load.start()
            value = packed(
                kern[g, ks].reshape(ks.size * rad_len, lat_len), pack_mat
            ).reshape(ks.size, rad_len, LANES)
        if p:
            g, ks = chunks[p - 1]
            high, low = halves(jnp.concatenate([before[k] for k in range(ks.size)], axis=1))
            done = jnp.dot(
                rad_mat[...], jnp.concatenate([high, low, high], axis=0),
                preferred_element_type=jnp.float32,
            )
            for k in range(ks.size):
                rad[g, ks.start + k] = done[:, k * LANES : (k + 1) * LANES]
            if p == 1:
                enter()
            exchange(p - 1)
    strips = part // SUB

    matrix = spread_out * jnp.sum(spread_out, axis=0, keepdims=True)
    high, low = halves(spread_out / jnp.sum(matrix, axis=1, keepdims=True))
    both = jnp.concatenate([high, low], axis=1)
    dual_mat[...] = jnp.concatenate([both, both], axis=0)
    matrix = factor((LANES, lat_len), 1, lat_len, 4.0, LANES)
    whole = jnp.sum(matrix * jnp.sum(matrix, axis=1, keepdims=True), axis=0, keepdims=True)
    high, low = halves(matrix / whole)
    lat_mat[...] = jnp.concatenate([high, high, low], axis=0)

    for copy, p in zip(far_copies, range(1, LOADS)):
        g, ks = chunks[p]
        copy.wait_recv()
        far_out[g, ks] = rad[g, ks, rows(far)] + far_in[g, ks]
        x_copies.append(send(
            far_out.at[g, ks], x_in.at[g, ks], x_send.at[p + 1], x_recv.at[p + 1],
            {"event": far},
        ))
        x_copies[-1].start()
    pass_right()

    slots = {pair: number for number, pair in enumerate(upper(pairs))}
    count = len(slots)
    groups = [(0, 1), (2, 3), tuple(range(4, pairs))]
    all_rows = steps.shape[1]
    tiles = all_rows // SUB
    lats = lat_len // LANES
    strip = tiles // UNITS

    def gram(number):
        if number == 0:
            loads[LOADS].wait()
            loads[LOADS + 1].wait()

        def scale(t, _):
            place = pl.ds(pl.multiple_of(t * SUB, SUB), SUB)
            for i in range(pairs):
                changes[i, place, :] = changes[i, place, :] * steps[i, place, :]
            return 0

        lax.fori_loop(number * strip, (number + 1) * strip, scale, 0, unroll=2)
        for group in groups:
            wanted = [(i, j) for i in group for j in range(i, pairs)]

            def body(t, sums):
                place = pl.ds(pl.multiple_of(t * SUB, SUB), SUB)
                sums = list(sums)
                for lane in range(lats):
                    across = pl.ds(lane * LANES, LANES)
                    change = {j: changes[j, place, across] for j in range(group[0], pairs)}
                    for n, i in enumerate(group):
                        step = steps[i, place, across]
                        for m, (a, b) in enumerate(wanted):
                            if a == i:
                                sums[2 * m] = sums[2 * m] + step * change[b]
                                sums[2 * m + 1] = sums[2 * m + 1] + change[i] * change[b]
                return tuple(sums)

            sums = lax.fori_loop(
                number * strip, (number + 1) * strip, body,
                tuple(jnp.zeros((SUB, LANES), jnp.float32) for _ in range(2 * len(wanted))),
            )
            for m, pair in enumerate(wanted):
                for kind in range(2):
                    place = slots[pair] + kind * count
                    if number == 0:
                        gram_acc[place] = sums[2 * m + kind]
                    else:
                        gram_acc[place] = gram_acc[place] + sums[2 * m + kind]

    def spread(row, slot_refs, sent, landed):
        for d, other in enumerate(others):
            send(row, slot_refs.at[d], sent, landed, other).start()
        return send(slot_refs, slot_refs, sent, landed, others[0])

    def gathered(row, slot_refs, copy):
        copy.wait_recv()
        return row[...] + jnp.sum(slot_refs[...], axis=0)

    near_all = send(near_in, near_in, core_send.at[0], core_recv.at[0], {"event": core})

    def arrive(p):
        g, ks = chunks[p]
        if p == 0:
            near_all.wait_recv()
        base = rad[g, ks, rows(e)] + near_in[g, ks]
        if p == 0:
            x_copies[0].wait_recv()
            x_copies[1].wait_recv()
            base = base + cross_in[...]
        else:
            x_copies[p + 1].wait_recv()
        nodes[g, ks] = base + x_in[g, ks]
        halo_copies.append(send(
            nodes.at[g, ks], halo_in.at[g, ks], halo_send.at[CHUNKS[p][0]], halo_recv.at[CHUNKS[p][0]],
            {"cuts": lax.rem(c + n_c - 1 + 2 * g, n_c)},
        ))
        halo_copies[-1].start()

    def shorten(kind, vector, first, last):
        for i in range(first, last, 2):
            place = pl.ds(kind * pairs + i, 2)
            short[place] = packed(
                vector[pl.ds(i, 2)].reshape(2 * all_rows, lat_len), dual_mat
            ).reshape(2, all_rows, LANES)

    weights = cycle_weights()

    def finish(turn):
        g = sides[turn]
        halo_all = send(
            halo_in.at[1 - g], halo_in.at[1 - g], halo_send.at[turn], halo_recv.at[turn],
            {"event": core},
        )
        halo_all.wait_recv()
        halo_all.wait_send()

        def at(k):
            return k + g * (RIM - 1 - 2 * k)

        sums = [None] * (2 * pairs)
        for h in range(strips):
            place = pl.ds(h * SUB, SUB)
            padded = (
                [halo_in[1 - g, at(k), place] for k in range(RIM)]
                + [nodes[g, at(k), place] for k in range(RIM)]
                + [nodes[1 - g, at(k), place] for k in range(RIM)]
            )
            for a in range(RIM):
                value = weights[RIM] * padded[a + RIM]
                for k in range(1, RIM + 1):
                    value = value + weights[RIM + k] * (padded[a + RIM - k] + padded[a + RIM + k])
                spot = pl.ds(pl.multiple_of((g * RIM + at(a)) * part + h * SUB, SUB), SUB)
                smooth[spot, :] = value
                for n in range(2 * pairs):
                    term = value * short[n, spot, :]
                    sums[n] = term if sums[n] is None else sums[n] + term
        for n in range(2 * pairs):
            place = pl.ds(n * SUB, SUB)
            table[place, :] = sums[n] if turn == 0 else table[place, :] + sums[n]

    pass_left()
    end_left()
    begun = 0
    for p in range(LOADS):
        arrive(p)
        if p < 3:
            gram(p)
        else:
            shorten(0, steps, begun, begun + 2)
            begun += 2
    for number in range(3, UNITS):
        gram(number)
    ones = jnp.ones((LANES, LANES), jnp.float32)

    def lane_sums(value):
        return lax.dot_general(
            ones[:SUB], value, (((1,), (1,)), ((), ())), precision=HIGHEST,
            preferred_element_type=jnp.float32,
        )[:1]

    table[pl.ds(0, 2 * count), :] = jnp.sum(gram_acc[...], axis=1)
    gram_row[...] = lane_sums(table[...])
    pl.semaphore_wait(ready.at[2], 1)
    gram_copies = spread(gram_row, gram_all, gram_send.at[0], gram_recv.at[0])
    shorten(0, steps, begun, pairs)
    shorten(1, changes, 0, pairs)
    finish(0)
    finish(1)
    first, _ = halves(table[...])
    second, third = halves(table[...] - first.astype(jnp.float32))
    late_row[...] = lax.dot_general(
        jnp.ones((SUB, 3 * LANES), jnp.bfloat16), jnp.concatenate([first, second, third], axis=1),
        (((1,), (1,)), ((), ())), preferred_element_type=jnp.float32,
    )[:1]
    late_copies = spread(late_row, late_all, late_send.at[0], late_recv.at[0])
    high, low = halves(smooth[...])
    grad[...] = jnp.dot(
        jnp.concatenate([high, low, high], axis=1), lat_mat[...],
        preferred_element_type=jnp.float32,
    )
    products = gathered(gram_row, gram_all, gram_copies)
    square = (LANES, LANES)
    on_diagonal = lax.broadcasted_iota(jnp.int32, square, 0) == lax.broadcasted_iota(jnp.int32, square, 1)
    splat[...] = jnp.dot(
        jnp.where(on_diagonal, jnp.broadcast_to(products, square), 0.0), ones,
        precision=HIGHEST, preferred_element_type=jnp.float32,
    )

    def cross(i, j):
        place = slots[i, j]
        return splat[place : place + 1, :]

    def squared(i, j):
        place = count + slots[min(i, j), max(i, j)]
        return splat[place : place + 1, :]

    def unit(place):
        return (lax.broadcasted_iota(jnp.int32, (1, LANES), 1) // SUB == place).astype(jnp.float32)

    inverse = [1.0 / cross(i, i) for i in range(pairs)]
    scaling = cross(pairs - 1, pairs - 1) / squared(pairs - 1, pairs - 1)
    alphas = [None] * pairs
    for i in reversed(range(pairs)):
        row = unit(i)
        for j in range(pairs - 1, i, -1):
            row = row - cross(i, j) * alphas[j]
        alphas[i] = inverse[i] * row
    onto = []
    for i in range(pairs):
        row = unit(pairs + i)
        for j in range(pairs):
            row = row - squared(i, j) * alphas[j]
        row = scaling * row
        for j in range(i):
            row = row + cross(j, i) * onto[j]
        onto.append(alphas[i] - inverse[i] * row)
    for i in range(pairs):
        mix[i : i + 1, :] = -onto[i]
        mix[pairs + i : pairs + i + 1, :] = scaling * alphas[i]

    for copies in (far_copies, x_copies, (near_all, gram_copies, late_copies)):
        for copy in copies:
            copy.wait_send()
    products = gathered(late_row, late_all, late_copies)
    mixed = jnp.sum(mix[...] * products, axis=1, keepdims=True)
    factors = [
        jnp.broadcast_to(mixed[i : i + 1], (SUB, LANES)) for i in range(2 * pairs)
    ]
    ratio = jnp.broadcast_to(-scaling, (SUB, LANES))

    def combine(t, _):
        place = pl.ds(pl.multiple_of(t * SUB, SUB), SUB)
        for lane in range(lats):
            across = pl.ds(lane * LANES, LANES)
            values = [ratio * grad[place, across]]
            for i in range(pairs):
                values.append(factors[i] * steps[i, place, across])
                values.append(factors[pairs + i] * changes[i, place, across])
            while len(values) > 1:
                paired = [x + y for x, y in zip(values[::2], values[1::2])]
                values = paired + values[2 * len(paired) :]
            direc[place, across] = values[0]
        return 0

    lax.fori_loop(0, tiles, combine, 0, unroll=8)


def shards(kernels, steps, curvature):
    n_c, n_e = lax.axis_size("cuts"), lax.axis_size("event")
    _, lons, rad_len, lat_len = kernels.shape
    pairs = steps.shape[0]
    part = rad_len // n_e
    assert lons == 2 * RIM and n_e == 4 and n_c % 2 == 0
    all_rows = lons * part
    count = pairs * (pairs + 1)
    f32, bf16 = jnp.float32, jnp.bfloat16
    vmem, dma = pltpu.VMEM, pltpu.SemaphoreType.DMA
    whole = (2, RIM, part, LANES)
    vmem_spec = pl.BlockSpec(memory_space=pltpu.VMEM)
    any_spec = pl.BlockSpec(memory_space=pl.ANY)
    others = n_c * n_e - 1
    assert 2 * pairs * SUB == LANES
    outs = pl.pallas_call(
        functools.partial(kernel, (n_c, n_e, pairs, rad_len, lat_len)),
        out_shape=vmem((2, all_rows, lat_len), f32),
        in_specs=[any_spec] * 3,
        out_specs=vmem_spec,
        scratch_shapes=[
            vmem((pairs, all_rows, lat_len), f32),
            vmem((pairs, all_rows, lat_len), f32),
            vmem((2, RIM, rad_len, lat_len), f32),
            vmem((2, RIM, rad_len, LANES), f32),
            vmem(whole, f32),
            vmem(whole, f32),
            vmem(whole, f32),
            vmem(whole, f32),
            vmem((CHUNKS[0][2], part, LANES), f32),
            vmem(whole, f32),
            vmem(whole, f32),
            vmem((all_rows, LANES), f32),
            vmem((2 * pairs, all_rows, LANES), f32),
            vmem((rad_len, 3 * rad_len), bf16),
            vmem((2 * lat_len, 2 * LANES), bf16),
            vmem((2 * lat_len, 2 * LANES), bf16),
            vmem((3 * LANES, lat_len), bf16),
            vmem((count, SUB, LANES), f32),
            vmem((1, LANES), f32),
            vmem((others, 1, LANES), f32),
            vmem((LANES, LANES), f32),
            vmem((LANES, LANES), f32),
            vmem((2 * pairs, LANES), f32),
            vmem((1, LANES), f32),
            vmem((others, 1, LANES), f32),
            pltpu.SemaphoreType.REGULAR((3,)),
            dma((LOADS + 2,)),
            dma((LOADS,)),
            dma((LOADS,)),
            dma((LOADS + 1,)),
            dma((LOADS + 1,)),
            dma((2,)),
            dma((2,)),
            dma((1,)),
            dma((1,)),
            dma((1,)),
            dma((1,)),
        ],
        compiler_params=pltpu.CompilerParams(
            collective_id=0, has_side_effects=True, vmem_limit_bytes=61905306
        ),
    )(
        kernels.reshape(2, RIM, rad_len, lat_len),
        steps.reshape(pairs, all_rows, lat_len),
        curvature.reshape(pairs, all_rows, lat_len),
    )
    shape = (lons, part, lat_len)
    return outs[0].reshape(shape), outs[1].reshape(shape)


def solution(mesh):
    placed = (
        P("event", "cuts", None, None),
        P(None, "cuts", "event", None),
        P(None, "cuts", "event", None),
    )
    return jax.shard_map(
        shards,
        mesh=mesh,
        in_specs=placed,
        out_specs=(P("cuts", "event", None), P("cuts", "event", None)),
        check_vma=False,
    )
```
